512 devices in a mesh: gx: 4 (over y_hi), gy: 16 (over z, y_lo), gz: 8 (over x, core).
Axes of the slice: x: 4, y: 8 (y_hi: 4, y_lo: 2; y = y_hi * 2 + y_lo), z: 8, core: 2. Of those that a mesh axis runs over, the one named last changes fastest.
Arguments:
- nodal_scalar_values: float32 [3, 32, 128, 16384], P(None, 'gx', 'gy', 'gz'), may hold values from -6 to 6
- geometry: float32 [6, 4, 16, 2048], P(None, 'gx', 'gy', 'gz'), may hold values from -1.2 to 4, as said below
Outputs:
- assembled: float32 [3, 32, 128, 16384], P(None, 'gx', 'gy', 'gz')
The draws below stay inside these ranges and needn't reach their ends.
Inputs may be any that keep to these rules, and one draw needn't show every extreme that they name: `geometry`: G00, G11 and G22 are positive; each off-diagonal factor is at most 0.3 times the root of the product of its two diagonal factors in magnitude.
All inputs are finite; a program needn't handle non-finite values.
Results may differ from the reference program's by a relative error of at most 0.00007.
Values sent between devices are 32-bit elements; how exact they have to be, the bound alone decides.
A program may use at most 64 MiB of HBM per device.

```python
import math
import jax
import jax.numpy as jnp
import numpy as np
from jax import lax

COMPONENTS = 3
ELEMENTS_FIRST = 4
ELEMENTS_SECOND = 16
ELEMENTS_THIRD = 2048


def draw_geometry(key, part):
    element_grid_shape = (ELEMENTS_FIRST, ELEMENTS_SECOND, ELEMENTS_THIRD)
    key_list = jax.random.split(key, 2)
    diagonal = jnp.exp(jax.random.uniform(key_list[0], (3,) + element_grid_shape, jnp.float32, math.log(0.5), math.log(2.0)))
    coupling = jax.random.uniform(key_list[1], (3,) + element_grid_shape, jnp.float32, -0.3, 0.3)
    cross_xy = coupling[0] * jnp.sqrt(diagonal[0] * diagonal[1])
    cross_xz = coupling[1] * jnp.sqrt(diagonal[0] * diagonal[2])
    cross_yz = coupling[2] * jnp.sqrt(diagonal[1] * diagonal[2])
    return jnp.stack([diagonal[0], diagonal[1], diagonal[2], cross_xy, cross_xz, cross_yz]).astype(jnp.float32)


def level_of(own_key, extent, cuts, low, high):
    factor_of, own = 1.0, jax.random.fold_in(own_key, 6)
    for axis_at, blocks in cuts:
        steps = jnp.exp(jax.random.uniform(jax.random.fold_in(own, axis_at), (blocks,), jnp.float32, low / len(cuts), high / len(cuts)))
        factor_of = factor_of * jnp.repeat(steps, extent[axis_at] // blocks).reshape([-1 if axis == axis_at else 1 for axis in range(len(extent))])
    return factor_of


def gaussian(key, shape, scale, most, pieces=(), held_as=jnp.bfloat16):
    level = level_of(key, shape, pieces, -0.22, 0.18) if pieces else 1.0
    entries = jax.random.normal(key, shape, jnp.float32) * scale * level
    return jnp.minimum(jnp.maximum(entries, -most), most).astype(held_as)


def setup_inputs(seed: int = 0) -> dict:
    key_of = jax.random.split(jax.random.key(seed), 3)
    return {
        "nodal_scalar_values": gaussian(key_of[0], (COMPONENTS, 8 * ELEMENTS_FIRST, 8 * ELEMENTS_SECOND, 8 * ELEMENTS_THIRD), 1.0, 6.0, ((1, 4), (2, 16), (3, 8)), jnp.float32),
        "geometry": draw_geometry(jax.random.fold_in(key_of[2], 71), 0),
    }


interior_points = [-0.8717401485096066, -0.5917001814331423, -0.2092992179024789, 0.2092992179024789, 0.5917001814331423, 0.8717401485096066]


def legendre_seven(point):
    previous = 1.0
    current = point
    for order in range(1, 7):
        following = ((2 * order + 1) * point * current - order * previous) / (order + 1)
        previous = current
        current = following
    return current


def gll_tables():
    degree = 7
    points = [-1.0] + interior_points + [1.0]
    values = [legendre_seven(point) for point in points]
    node_count = degree + 1
    weights = np.array([2.0 / (degree * (degree + 1) * value * value) for value in values])
    derivative = np.zeros((node_count, node_count))
    for row_index in range(node_count):
        for col_index in range(node_count):
            if row_index != col_index:
                derivative[row_index, col_index] = values[row_index] / (values[col_index] * (points[row_index] - points[col_index]))
    derivative[0, 0] = -degree * (degree + 1) / 4.0
    derivative[node_count - 1, node_count - 1] = degree * (degree + 1) / 4.0
    return derivative, weights


def apply_axis(field_in, matrix, direction):
    length = field_in.shape[direction]
    block_size = math.gcd(length, 128)
    big_table = jnp.kron(jnp.eye(block_size // 8, dtype=jnp.float32), matrix)
    dim_list = list(field_in.shape)
    folded_shape = dim_list[:direction] + [length // block_size, block_size] + dim_list[direction + 1:]
    folded_field = field_in.reshape(folded_shape)
    patterns = ["nbyz,ab->nayz", "xnbz,ab->xnaz", "xynb,ab->xyna"]
    result = jnp.einsum(patterns[direction], folded_field, big_table, precision=lax.Precision.HIGHEST)
    return result.reshape(field_in.shape)


def expand(field_component, target):
    elem_x, elem_y, elem_z = field_component.shape
    spread = jnp.broadcast_to(field_component[:, None, :, None, :, None], (elem_x, 8, elem_y, 8, elem_z, 8))
    return spread.reshape(target)


def stiffness(field_in, geometry):
    derivative, weights = gll_tables()
    matrix = jnp.asarray(derivative, jnp.float32)
    weight_row = jnp.asarray(weights, jnp.float32)
    size_x, size_y, size_z = field_in.shape
    weight_x = jnp.tile(weight_row, size_x // 8)
    weight_y = jnp.tile(weight_row, size_y // 8)
    weight_z = jnp.tile(weight_row, size_z // 8)
    node_weight = weight_x[:, None, None] * weight_y[None, :, None] * weight_z[None, None, :]
    grad_x = apply_axis(field_in, matrix, 0)
    grad_y = apply_axis(field_in, matrix, 1)
    grad_z = apply_axis(field_in, matrix, 2)
    factors = [expand(geometry[index], field_in.shape) for index in range(6)]
    flux_x = node_weight * (factors[0] * grad_x + factors[3] * grad_y + factors[4] * grad_z)
    flux_y = node_weight * (factors[3] * grad_x + factors[1] * grad_y + factors[5] * grad_z)
    flux_z = node_weight * (factors[4] * grad_x + factors[5] * grad_y + factors[2] * grad_z)
    transposed = matrix.T
    return apply_axis(flux_x, transposed, 0) + apply_axis(flux_y, transposed, 1) + apply_axis(flux_z, transposed, 2)


def combine(middle, below_plane, above_plane, direction):
    length = middle.shape[direction]
    from_above = jnp.concatenate([lax.slice_in_dim(middle, 1, length, axis=direction), above_plane], axis=direction)
    from_below = jnp.concatenate([below_plane, lax.slice_in_dim(middle, 0, length - 1, axis=direction)], axis=direction)
    position = lax.broadcasted_iota(jnp.int32, middle.shape, direction) % 8
    return middle + jnp.where(position == 7, from_above, 0.0) + jnp.where(position == 0, from_below, 0.0)


def single_component(field_values, geometry):
    total_x, total_y, total_z = field_values.shape
    zblock = math.gcd(total_z, 1024)
    block_count = total_z // zblock
    field_blocks = jnp.moveaxis(field_values.reshape(total_x, total_y, block_count, zblock), 2, 0)
    geometries = jnp.moveaxis(geometry.reshape(6, geometry.shape[1], geometry.shape[2], block_count, zblock // 8), 3, 0)
    local_terms = lax.map(lambda operands: stiffness(operands[0], operands[1]), (field_blocks, geometries))
    local_terms = jnp.moveaxis(local_terms, 0, 2).reshape(field_values.shape)
    summed = local_terms
    for direction in range(3):
        plane_extents = list(summed.shape)
        plane_extents[direction] = 1
        zero_plane = jnp.zeros(plane_extents, jnp.float32)
        summed = combine(summed, zero_plane, zero_plane, direction)
    return summed


def reference(nodal_scalar_values, geometry):
    return jnp.stack([single_component(nodal_scalar_values[component], geometry) for component in range(COMPONENTS)])
```

```python
import functools

import jax
import jax.numpy as jnp
import numpy as np
from jax import lax
from jax.experimental import pallas as pl
from jax.experimental.pallas import tpu as pltpu
from jax.sharding import PartitionSpec as P

interior_points = [
    -0.8717401485096066,
    -0.5917001814331423,
    -0.2092992179024789,
    0.2092992179024789,
    0.5917001814331423,
    0.8717401485096066,
]
MESH = pl.DeviceIdType.MESH
CHUNK = 256
WIDE = 512
LANES = 128


def legendre_seven(point):
    previous = 1.0
    current = point
    for order in range(1, 7):
        following = ((2 * order + 1) * point * current - order * previous) / (order + 1)
        previous = current
        current = following
    return current


def gll_tables():
    degree = 7
    points = [-1.0] + interior_points + [1.0]
    values = [legendre_seven(point) for point in points]
    node_count = degree + 1
    weights = np.array([2.0 / (degree * (degree + 1) * value * value) for value in values])
    derivative = np.zeros((node_count, node_count))
    for row_index in range(node_count):
        for col_index in range(node_count):
            if row_index != col_index:
                derivative[row_index, col_index] = values[row_index] / (
                    values[col_index] * (points[row_index] - points[col_index])
                )
    derivative[0, 0] = -degree * (degree + 1) / 4.0
    derivative[node_count - 1, node_count - 1] = degree * (degree + 1) / 4.0
    return (derivative, weights)


def halves(table):
    table = np.asarray(table, np.float32)
    high = table.astype(jnp.bfloat16)
    low = (table - high.astype(np.float32)).astype(jnp.bfloat16)
    return high, low


def tables():
    derivative, weights = gll_tables()
    eye = np.eye(8)
    plane_weight = np.kron(weights, weights)
    forward_xy = np.concatenate([np.kron(derivative, eye), np.kron(eye, derivative)], axis=0)
    back_xy = np.concatenate([np.kron(derivative.T, eye), np.kron(eye, derivative.T)], axis=1)
    back_xy = back_xy * np.tile(plane_weight, 2)[None, :]
    forward_z = np.kron(np.eye(16), derivative.T)
    back_z = np.kron(np.eye(16), derivative)
    high, low = halves(forward_xy)
    forward_xy = np.concatenate([high, high, low, low], axis=1)
    high, low = halves(back_xy)
    back_xy = np.concatenate(
        [np.concatenate([high, high], axis=1), np.concatenate([low, low], axis=1)], axis=0
    )
    high, low = halves(forward_z)
    forward_z = np.tile(np.concatenate([high, low], axis=1), (2, 1))
    high, low = halves(back_z)
    back_z = np.tile(np.concatenate([high, low], axis=1), (2, 1))
    matrices = np.concatenate([forward_xy, back_xy, forward_z, back_z], axis=0)
    plane = np.repeat(plane_weight[:, None], LANES, axis=1)
    along = np.repeat(np.tile(weights, LANES // 8)[None, :], 8, axis=0)
    scales = np.concatenate([plane, along], axis=0).astype(np.float32)
    return matrices, scales


def split(value):
    high = value.astype(jnp.bfloat16)
    low = (value - high.astype(jnp.float32)).astype(jnp.bfloat16)
    return high, low


def product(left, right):
    return jnp.dot(left, right, preferred_element_type=jnp.float32)


def along_lanes(high, low, table):
    pieces = []
    for start in range(0, high.shape[1], LANES):
        both = jnp.concatenate(
            [high[:, start : start + LANES], low[:, start : start + LANES]], axis=1
        )
        twice = product(both, table)
        pieces.append(twice[:, :LANES] + twice[:, LANES:])
    return jnp.concatenate(pieces, axis=1)


def kernel(
    sizes,
    u_hbm,
    geo_hbm,
    mat_hbm,
    scale_hbm,
    out,
    u,
    geo,
    mat,
    scale,
    local,
    x_in,
    mid_out,
    mid_in,
    edge_out,
    edge_in,
    z_out,
    z_in,
    in_sem,
    const_sem,
    x_send,
    x_recv,
    mid_send,
    mid_recv,
    edge_send,
    edge_recv,
    z_send,
    z_recv,
):
    comps, _, _, total = u.shape
    count = total // CHUNK
    wides = total // WIDE
    tiles = total // LANES
    per_wide = WIDE // CHUNK
    across = WIDE // LANES
    wide_order = [0] + ([wides - 1] if wides > 1 else []) + list(range(1, wides - 1))
    order = [w * per_wide + k for w in wide_order for k in range(per_wide)]
    names = ("gx", "gy", "gz")
    place = {name: lax.axis_index(name) for name in names}
    below = {name: place[name] > 0 for name in names}
    above = {name: place[name] < sizes[name] - 1 for name in names}

    const_copies = [
        pltpu.make_async_copy(geo_hbm, geo, const_sem.at[2]),
        pltpu.make_async_copy(scale_hbm, scale, const_sem.at[1]),
        pltpu.make_async_copy(mat_hbm, mat, const_sem.at[0]),
    ]
    for copy in const_copies:
        copy.start()
    in_copies = {}
    for c in order:
        span = pl.ds(c * CHUNK, CHUNK)
        in_copies[c] = pltpu.make_async_copy(
            u_hbm.at[:, :, :, span], u.at[:, :, :, span], in_sem.at[c]
        )
        in_copies[c].start()

    barrier = pltpu.get_barrier_semaphore()
    for name in names:
        for there, by in ((below[name], -1), (above[name], 1)):

            @pl.when(there)
            def _(name=name, by=by):
                pl.semaphore_signal(
                    barrier, inc=1, device_id={name: place[name] + by}, device_id_type=MESH
                )

    def target(name, side):
        return above[name] if side == 0 else below[name]

    def source(name, side):
        return below[name] if side == 0 else above[name]

    def when_do(condition, act):
        @pl.when(condition)
        def _():
            act()

    for side in range(2):

        @pl.when(jnp.logical_not(source("gx", side)))
        def _(side=side):
            x_in[side] = jnp.zeros(x_in.shape[1:], jnp.float32)

        @pl.when(jnp.logical_not(source("gy", side)))
        def _(side=side):
            mid_in[side] = jnp.zeros(mid_in.shape[1:], jnp.float32)
            edge_in[side] = jnp.zeros(edge_in.shape[1:], jnp.float32)

        @pl.when(jnp.logical_not(source("gz", side)))
        def _(side=side):
            z_in[side] = jnp.zeros(z_in.shape[1:], jnp.float32)

    def neighbour(name, side):
        return {name: place[name] + (1 if side == 0 else -1)}

    def x_copy(side, c):
        span = pl.ds(c * CHUNK, CHUNK)
        return pltpu.make_async_remote_copy(
            local.at[:, 7 if side == 0 else 0, :, span],
            x_in.at[side, :, :, span],
            x_send.at[side, c],
            x_recv.at[side, c],
            device_id=neighbour("gx", side),
            device_id_type=MESH,
        )

    def mid_copy(side, w):
        return pltpu.make_async_remote_copy(
            mid_out.at[side, w],
            mid_in.at[side, w],
            mid_send.at[side, w],
            mid_recv.at[side, w],
            device_id=neighbour("gy", side),
            device_id_type=MESH,
        )

    def edge_copy(side, w):
        return pltpu.make_async_remote_copy(
            edge_out.at[side, w],
            edge_in.at[side, w],
            edge_send.at[side, w],
            edge_recv.at[side, w],
            device_id=neighbour("gy", side),
            device_id_type=MESH,
        )

    def z_copy(side):
        return pltpu.make_async_remote_copy(
            z_out.at[side],
            z_in.at[side],
            z_send.at[side],
            z_recv.at[side],
            device_id=neighbour("gz", side),
            device_id_type=MESH,
        )

    def mid_row(comp, n, tile):
        return (comp * 6 + n - 1) * across + tile % across

    def edge_row(comp, end, tile):
        return (comp * 2 + end) * across + tile % across

    for copy in const_copies[:2]:
        copy.wait()
    rows = jnp.concatenate(
        [geo[k, 0] for k in range(6)] + [jnp.zeros((2, geo.shape[-1]), jnp.float32)], axis=0
    )
    lane = lax.broadcasted_iota(jnp.int32, (8, LANES), 1)

    def metric_of(tile):
        first = tile * (LANES // 8)
        block = rows[:, first // LANES * LANES : first // LANES * LANES + LANES]
        spread = jnp.take_along_axis(block, lane // 8 + first % LANES, axis=1)
        return spread * scale[64:72, :]

    def compute(c):
        start = c * CHUNK
        lanes = slice(start, start + CHUNK)
        metric = jnp.concatenate(
            [metric_of(start // LANES + k) for k in range(CHUNK // LANES)], axis=1
        )
        g00, g11, g22, g01, g02, g12 = [metric[k : k + 1] for k in range(6)]
        forward_xy, back_xy = mat[0:128, :], mat[128:256, :]
        forward_z, back_z = mat[256:512, :], mat[512:768, :]
        for comp in range(comps):
            field = u[comp, :, :, lanes].reshape(64, CHUNK)
            high, low = split(field)
            both = product(forward_xy, jnp.concatenate([high, low, high, low], axis=0))
            grad_x, grad_y = both[:64], both[64:]
            grad_z = along_lanes(high, low, forward_z)
            flux_x = g00 * grad_x + g01 * grad_y + g02 * grad_z
            flux_y = g01 * grad_x + g11 * grad_y + g12 * grad_z
            flux_z = g02 * grad_x + g12 * grad_y + g22 * grad_z
            x_high, x_low = split(flux_x)
            y_high, y_low = split(flux_y)
            z_high, z_low = split(flux_z)
            twice = product(back_xy, jnp.concatenate([x_high, y_high, x_low, y_low], axis=0))
            terms = twice[:64] + twice[64:]
            weight = jnp.concatenate([scale[0:64, :]] * (CHUNK // LANES), axis=1)
            terms = terms + weight * along_lanes(z_high, z_low, back_z)
            terms = terms.reshape(8, 8, CHUNK)
            local[comp, :, :, lanes] = terms
            for n in range(1, 7):
                for k in range(CHUNK // LANES):
                    tile = start // LANES + k
                    row = mid_row(comp, n, tile)
                    part = slice(k * LANES, (k + 1) * LANES)
                    mid_out[0, tile // across, row : row + 1, :] = terms[n, 7:8, part]
                    mid_out[1, tile // across, row : row + 1, :] = terms[n, 0:1, part]

    def corners(w):
        for c in range(w * per_wide, (w + 1) * per_wide):
            for side in range(2):
                when_do(source("gx", side), lambda: x_copy(side, c).wait_recv())
        for comp in range(comps):
            for end in range(2):
                for tile in range(w * across, (w + 1) * across):
                    lanes = slice(tile * LANES, (tile + 1) * LANES)
                    value = local[comp, 7 * end, :, lanes] + x_in[end, comp, :, lanes]
                    x_in[end, comp, :, lanes] = value
                    row = edge_row(comp, end, tile)
                    edge_out[0, w, row : row + 1, :] = value[7:8]
                    edge_out[1, w, row : row + 1, :] = value[0:1]
        for side in range(2):
            when_do(target("gy", side), lambda: edge_copy(side, w).start())

    def send_mid(w):
        for side in range(2):
            when_do(target("gy", side), lambda: mid_copy(side, w).start())

    def wait_mid(w):
        for side in range(2):
            when_do(source("gy", side), lambda: mid_copy(side, w).wait_recv())

    def wait_edge(w):
        for side in range(2):
            when_do(source("gy", side), lambda: edge_copy(side, w).wait_recv())

    def xy_sum(comp, n, tile):
        lanes = slice(tile * LANES, (tile + 1) * LANES)
        w = tile // across
        if n in (0, 7):
            value = x_in[n // 7, comp, :, lanes]
            row = edge_row(comp, n // 7, tile)
            sides = [edge_in[side, w, row : row + 1, :] for side in range(2)]
        else:
            value = local[comp, n, :, lanes]
            row = mid_row(comp, n, tile)
            sides = [mid_in[side, w, row : row + 1, :] for side in range(2)]
        where = lax.broadcasted_iota(jnp.int32, value.shape, 0)
        value = value + jnp.where(where == 0, sides[0], 0.0)
        return value + jnp.where(where == 7, sides[1], 0.0)

    def finish(which, first, last):
        for comp in range(comps):
            for n in which:
                parts = []
                for tile in range(first - 1, last + 1):
                    if tile < 0:
                        parts.append(z_in[0, comp, n])
                    elif tile == tiles:
                        parts.append(z_in[1, comp, n])
                    else:
                        parts.append(xy_sum(comp, n, tile))
                value = jnp.concatenate(parts, axis=1)
                width = value.shape[1]
                before = pltpu.roll(value, 1, 1)[:, LANES:-LANES]
                after = pltpu.roll(value, width - 1, 1)[:, LANES:-LANES]
                position = lax.broadcasted_iota(jnp.int32, before.shape, 1) % 8
                extra = jnp.where(position == 7, after, jnp.where(position == 0, before, 0.0))
                out[comp, n, :, first * LANES : last * LANES] = value[:, LANES:-LANES] + extra

    middle, ends = range(1, 7), (0, 7)
    z_here = []

    def wait_z():
        if not z_here:
            z_here.append(True)
            for side in range(2):
                when_do(source("gz", side), lambda: z_copy(side).wait_recv())

    finished = {middle: set(), ends: set()}
    arrived = {middle: set(), ends: set()}

    def finish_ready(which, with_z):
        have = arrived[which]

        def near(tile):
            return tile // across in have if 0 <= tile < tiles else with_z

        ready = [
            tile
            for tile in range(tiles)
            if tile not in finished[which] and all(near(tile + k) for k in (-1, 0, 1))
        ]
        while ready:
            first = last = ready.pop(0)
            while ready and ready[0] == last + 1 and last - first < across - 1:
                last = ready.pop(0)
            finished[which].update(range(first, last + 1))
            finish(which, first, last + 1)

    greeted = sum(side[name].astype(jnp.int32) for name in names for side in (below, above))
    const_copies[2].wait()
    for at, c in enumerate(order):
        in_copies[c].wait()
        compute(c)
        if at == 0:
            pl.semaphore_wait(barrier, greeted)
        for side in range(2):
            when_do(target("gx", side), lambda: x_copy(side, c).start())
        if at == 1:
            send_mid(wide_order[0])
        if at == 4:
            send_mid(wide_order[1])
        if at == 5:
            corners(wide_order[0])
    send_mid(wide_order[2])
    corners(wide_order[1])
    send_mid(wide_order[3])
    corners(wide_order[2])
    corners(wide_order[3])

    for w in wide_order[:2]:
        wait_mid(w)
        wait_edge(w)
        arrived[middle].add(w)
        arrived[ends].add(w)
    for side in range(2):
        tile = tiles - 1 if side == 0 else 0
        for comp in range(comps):
            for n in range(8):
                z_out[side, comp, n] = xy_sum(comp, n, tile)
        when_do(target("gz", side), lambda: z_copy(side).start())
    finish_ready(middle, False)
    finish_ready(ends, False)
    wait_mid(wide_order[2])
    arrived[middle].add(wide_order[2])
    finish_ready(middle, False)
    wait_edge(wide_order[2])
    arrived[ends].add(wide_order[2])
    finish_ready(ends, False)
    wait_z()
    finish_ready(middle, True)
    finish_ready(ends, True)
    wait_mid(wide_order[3])
    arrived[middle].add(wide_order[3])
    finish_ready(middle, True)
    wait_edge(wide_order[3])
    arrived[ends].add(wide_order[3])
    finish_ready(ends, True)

    for side in range(2):
        for c in order:
            when_do(target("gx", side), lambda: x_copy(side, c).wait_send())
        for w in wide_order:
            when_do(target("gy", side), lambda: mid_copy(side, w).wait_send())
            when_do(target("gy", side), lambda: edge_copy(side, w).wait_send())
        when_do(target("gz", side), lambda: z_copy(side).wait_send())


def local_part(sizes, nodal_scalar_values, geometry):
    comps, _, _, total = nodal_scalar_values.shape
    count = total // CHUNK
    wides = total // WIDE
    across = WIDE // LANES
    matrices, scales = tables()
    f32 = jnp.float32
    dma = pltpu.SemaphoreType.DMA
    any_space = pl.BlockSpec(memory_space=pl.ANY)
    return pl.pallas_call(
        functools.partial(kernel, sizes),
        out_shape=pltpu.VMEM(nodal_scalar_values.shape, f32),
        in_specs=[any_space] * 4,
        out_specs=pl.BlockSpec(memory_space=pltpu.VMEM),
        scratch_shapes=[
            pltpu.VMEM(nodal_scalar_values.shape, f32),
            pltpu.VMEM(geometry.shape, f32),
            pltpu.VMEM(matrices.shape, jnp.bfloat16),
            pltpu.VMEM(scales.shape, f32),
            pltpu.VMEM(nodal_scalar_values.shape, f32),
            pltpu.VMEM((2, comps, 8, total), f32),
            pltpu.VMEM((2, wides, comps * 6 * across, LANES), f32),
            pltpu.VMEM((2, wides, comps * 6 * across, LANES), f32),
            pltpu.VMEM((2, wides, comps * 2 * across, LANES), f32),
            pltpu.VMEM((2, wides, comps * 2 * across, LANES), f32),
            pltpu.VMEM((2, comps, 8, 8, LANES), f32),
            pltpu.VMEM((2, comps, 8, 8, LANES), f32),
            dma((count,)),
            dma((3,)),
            dma((2, count)),
            dma((2, count)),
            dma((2, wides)),
            dma((2, wides)),
            dma((2, wides)),
            dma((2, wides)),
            dma((2,)),
            dma((2,)),
        ],
        compiler_params=pltpu.CompilerParams(collective_id=0, has_side_effects=True),
        name="poisson",
    )(nodal_scalar_values, geometry, jnp.asarray(matrices), jnp.asarray(scales))


def solution(mesh):
    return jax.shard_map(
        functools.partial(local_part, dict(mesh.shape)),
        mesh=mesh,
        in_specs=(P(None, "gx", "gy", "gz"), P(None, "gx", "gy", "gz")),
        out_specs=P(None, "gx", "gy", "gz"),
        check_vma=False,
    )
```

```python
import functools

import jax
import jax.numpy as jnp
import numpy as np
from jax import lax
from jax.experimental import pallas as pl
from jax.experimental.pallas import tpu as pltpu
from jax.sharding import PartitionSpec as P

interior_points = [
    -0.8717401485096066,
    -0.5917001814331423,
    -0.2092992179024789,
    0.2092992179024789,
    0.5917001814331423,
    0.8717401485096066,
]
MESH = pl.DeviceIdType.MESH
CHUNK = 256
LANES = 128
PER = CHUNK // LANES
GROUP = 4


def plan(total):
    count, tiles = total // CHUNK, total // LANES
    order = [0, count - 1] + list(range(1, count - 1))
    rest = [c * PER + k for c in order for k in range(PER)]
    return order, [rest[at : at + GROUP] for at in range(0, tiles, GROUP)]


def offsets(groups, rows):
    places, at = [], 0
    for group in groups:
        size = -(-len(group) * rows // 8) * 8
        places.append((at, size))
        at += size
    return places, at


def legendre_seven(point):
    previous = 1.0
    current = point
    for order in range(1, 7):
        following = ((2 * order + 1) * point * current - order * previous) / (order + 1)
        previous = current
        current = following
    return current


def gll_tables():
    degree = 7
    points = [-1.0] + interior_points + [1.0]
    values = [legendre_seven(point) for point in points]
    node_count = degree + 1
    weights = np.array([2.0 / (degree * (degree + 1) * value * value) for value in values])
    derivative = np.zeros((node_count, node_count))
    for row_index in range(node_count):
        for col_index in range(node_count):
            if row_index != col_index:
                derivative[row_index, col_index] = values[row_index] / (
                    values[col_index] * (points[row_index] - points[col_index])
                )
    derivative[0, 0] = -degree * (degree + 1) / 4.0
    derivative[node_count - 1, node_count - 1] = degree * (degree + 1) / 4.0
    return (derivative, weights)


def halves(table):
    table = np.asarray(table, np.float32)
    high = table.astype(jnp.bfloat16)
    low = (table - high.astype(np.float32)).astype(jnp.bfloat16)
    return high, low


def tables():
    derivative, weights = gll_tables()
    eye = np.eye(8)
    plane_weight = np.kron(weights, weights)
    forward_xy = np.concatenate([np.kron(derivative, eye), np.kron(eye, derivative)], axis=0)
    back_xy = np.concatenate([np.kron(derivative.T, eye), np.kron(eye, derivative.T)], axis=1)
    back_xy = back_xy * np.tile(plane_weight, 2)[None, :]
    forward_z = np.kron(np.eye(16), derivative.T)
    back_z = np.kron(np.eye(16), derivative)
    high, low = halves(forward_xy)
    forward_xy = np.concatenate([high, high, low, low], axis=1)
    high, low = halves(back_xy)
    back_xy = np.concatenate(
        [np.concatenate([high, high], axis=1), np.concatenate([low, low], axis=1)], axis=0
    )
    high, low = halves(forward_z)
    forward_z = np.concatenate([high, low], axis=1)
    high, low = halves(back_z)
    back_z = np.concatenate([high, low], axis=1)
    matrices = np.concatenate([forward_xy, back_xy, forward_z, back_z], axis=0)
    plane = np.repeat(plane_weight[:, None], LANES, axis=1)
    along = np.repeat(np.tile(weights, LANES // 8)[None, :], 8, axis=0)
    scales = np.concatenate([plane, along], axis=0).astype(np.float32)
    return matrices, scales


def split(value):
    high = value.astype(jnp.bfloat16)
    low = (value - high.astype(jnp.float32)).astype(jnp.bfloat16)
    return high, low


def product(left, right):
    return jnp.dot(left, right, preferred_element_type=jnp.float32)


def along_lanes(high, low, table):
    pieces = []
    for start in range(0, high.shape[1], LANES):
        both = jnp.concatenate(
            [high[:, start : start + LANES], low[:, start : start + LANES]], axis=1
        )
        twice = product(both, table)
        pieces.append(twice[:, :LANES] + twice[:, LANES:])
    return jnp.concatenate(pieces, axis=1)


def kernel(
    sizes,
    u_hbm,
    geo_hbm,
    mat_hbm,
    scale_hbm,
    out,
    u,
    geo,
    mat,
    scale,
    local,
    x_in,
    mid_out,
    mid_in,
    edge_out,
    edge_in,
    z_out,
    z_in,
    in_sem,
    const_sem,
    x_send,
    x_recv,
    mid_send,
    mid_recv,
    edge_send,
    edge_recv,
    z_send,
    z_recv,
):
    comps, _, _, total = u.shape
    tiles = total // LANES
    order, groups = plan(total)
    mid_place, _ = offsets(groups, comps * 6)
    edge_place, _ = offsets(groups, comps * 2)
    group_of = {tile: (g, k) for g, group in enumerate(groups) for k, tile in enumerate(group)}
    names = ("gx", "gy", "gz")
    place = {name: lax.axis_index(name) for name in names}
    below = {name: place[name] > 0 for name in names}
    above = {name: place[name] < sizes[name] - 1 for name in names}

    def in_copy(at, first, last):
        span = pl.ds(first * CHUNK, (last - first) * CHUNK)
        return pltpu.make_async_copy(
            u_hbm.at[:, :, :, span], u.at[:, :, :, span], in_sem.at[at]
        )

    count = total // CHUNK
    in_copies = [in_copy(0, 0, 1), in_copy(1, count - 1, count), in_copy(2, 1, count - 1)]
    const_copies = [
        pltpu.make_async_copy(geo_hbm, geo, const_sem.at[0]),
        pltpu.make_async_copy(scale_hbm, scale, const_sem.at[1]),
        pltpu.make_async_copy(mat_hbm, mat, const_sem.at[2]),
    ]
    in_copies[0].start()
    for copy in const_copies:
        copy.start()

    barrier = pltpu.get_barrier_semaphore()
    for name in names:
        for there, by in ((below[name], -1), (above[name], 1)):

            @pl.when(there)
            def _(name=name, by=by):
                pl.semaphore_signal(
                    barrier, inc=1, device_id={name: place[name] + by}, device_id_type=MESH
                )

    for copy in in_copies[1:]:
        copy.start()

    def target(name, side):
        return above[name] if side == 0 else below[name]

    def source(name, side):
        return below[name] if side == 0 else above[name]

    def when_do(condition, act):
        @pl.when(condition)
        def _():
            act()

    for side in range(2):

        @pl.when(jnp.logical_not(source("gx", side)))
        def _(side=side):
            x_in[side] = jnp.zeros(x_in.shape[1:], jnp.float32)

        @pl.when(jnp.logical_not(source("gy", side)))
        def _(side=side):
            mid_in[side] = jnp.zeros(mid_in.shape[1:], jnp.float32)
            edge_in[side] = jnp.zeros(edge_in.shape[1:], jnp.float32)

        @pl.when(jnp.logical_not(source("gz", side)))
        def _(side=side):
            z_in[side] = jnp.zeros(z_in.shape[1:], jnp.float32)

    def neighbour(name, side):
        return {name: place[name] + (1 if side == 0 else -1)}

    def x_copy(side, first, size):
        span = pl.ds(first, size)
        return pltpu.make_async_remote_copy(
            local.at[:, 7 if side == 0 else 0, :, span],
            x_in.at[side, :, :, span],
            x_send,
            x_recv.at[first // CHUNK],
            device_id=neighbour("gx", side),
            device_id_type=MESH,
        )

    def mid_copy(side, g):
        span = pl.ds(*mid_place[g])
        return pltpu.make_async_remote_copy(
            mid_out.at[side, span],
            mid_in.at[side, span],
            mid_send,
            mid_recv.at[g],
            device_id=neighbour("gy", side),
            device_id_type=MESH,
        )

    def edge_copy(side, g):
        span = pl.ds(*edge_place[g])
        return pltpu.make_async_remote_copy(
            edge_out.at[side, span],
            edge_in.at[side, span],
            edge_send,
            edge_recv.at[g],
            device_id=neighbour("gy", side),
            device_id_type=MESH,
        )

    def z_copy(side):
        return pltpu.make_async_remote_copy(
            z_out.at[side],
            z_in.at[side],
            z_send,
            z_recv,
            device_id=neighbour("gz", side),
            device_id_type=MESH,
        )

    def take_both(name, ref, part, semaphore):
        both = jnp.logical_and(below[name], above[name])
        one = jnp.logical_xor(below[name], above[name])
        for condition, sides in ((both, 2), (one, 1)):
            piece = ref.at[(pl.ds(0, sides),) + part]
            when_do(condition, lambda: pltpu.make_async_copy(piece, piece, semaphore).wait())

    def mid_row(comp, n, tile):
        g, k = group_of[tile]
        return mid_place[g][0] + k * comps * 6 + comp * 6 + n - 1

    def edge_row(comp, end, tile):
        g, k = group_of[tile]
        return edge_place[g][0] + k * comps * 2 + comp * 2 + end

    for copy in const_copies[:2]:
        copy.wait()
    rows = jnp.concatenate(
        [geo[k, 0] for k in range(6)] + [jnp.zeros((2, geo.shape[-1]), jnp.float32)], axis=0
    )
    lane = lax.broadcasted_iota(jnp.int32, (8, LANES), 1)

    def metric_of(tile):
        first = tile * (LANES // 8)
        block = rows[:, first // LANES * LANES : first // LANES * LANES + LANES]
        spread = jnp.take_along_axis(block, lane // 8 + first % LANES, axis=1)
        return spread * scale[64:72, :]

    def compute(start, size):
        lanes = slice(start, start + size)
        metric = jnp.concatenate(
            [metric_of(start // LANES + k) for k in range(size // LANES)], axis=1
        )
        g00, g11, g22, g01, g02, g12 = [metric[k : k + 1] for k in range(6)]
        forward_xy, back_xy = mat[0:128, :], mat[128:256, :]
        forward_z = jnp.concatenate([mat[256:384, :]] * 2, axis=0)
        back_z = jnp.concatenate([mat[384:512, :]] * 2, axis=0)
        for comp in range(comps):
            field = u[comp, :, :, lanes].reshape(64, size)
            high, low = split(field)
            both = product(forward_xy, jnp.concatenate([high, low, high, low], axis=0))
            grad_x, grad_y = both[:64], both[64:]
            grad_z = along_lanes(high, low, forward_z)
            flux_x = g00 * grad_x + g01 * grad_y + g02 * grad_z
            flux_y = g01 * grad_x + g11 * grad_y + g12 * grad_z
            flux_z = g02 * grad_x + g12 * grad_y + g22 * grad_z
            x_high, x_low = split(flux_x)
            y_high, y_low = split(flux_y)
            z_high, z_low = split(flux_z)
            twice = product(back_xy, jnp.concatenate([x_high, y_high, x_low, y_low], axis=0))
            terms = twice[:64] + twice[64:]
            weight = jnp.concatenate([scale[0:64, :]] * (size // LANES), axis=1)
            terms = terms + weight * along_lanes(z_high, z_low, back_z)
            terms = terms.reshape(8, 8, size)
            local[comp, :, :, lanes] = terms
            for n in range(1, 7):
                for k in range(size // LANES):
                    row = mid_row(comp, n, start // LANES + k)
                    part = slice(k * LANES, (k + 1) * LANES)
                    mid_out[0, row : row + 1, :] = terms[n, 7:8, part]
                    mid_out[1, row : row + 1, :] = terms[n, 0:1, part]

    x_here = set()

    def wait_x(c):
        if c not in x_here:
            x_here.add(c)
            span = pl.ds(c * CHUNK, CHUNK)
            take_both("gx", x_in, (slice(None), slice(None), span), x_recv.at[c])

    def corners(g):
        for tile in groups[g]:
            wait_x(tile // PER)
        for comp in range(comps):
            for end in range(2):
                for tile in groups[g]:
                    lanes = slice(tile * LANES, (tile + 1) * LANES)
                    value = local[comp, 7 * end, :, lanes] + x_in[end, comp, :, lanes]
                    x_in[end, comp, :, lanes] = value
                    row = edge_row(comp, end, tile)
                    edge_out[0, row : row + 1, :] = value[7:8]
                    edge_out[1, row : row + 1, :] = value[0:1]
        for side in range(2):
            when_do(target("gy", side), lambda: edge_copy(side, g).start())

    def send_mid(g):
        for side in range(2):
            when_do(target("gy", side), lambda: mid_copy(side, g).start())

    def wait_mid(g):
        take_both("gy", mid_in, (pl.ds(*mid_place[g]),), mid_recv.at[g])

    def wait_edge(g):
        take_both("gy", edge_in, (pl.ds(*edge_place[g]),), edge_recv.at[g])

    def xy_sum(comp, n, tile):
        lanes = slice(tile * LANES, (tile + 1) * LANES)
        if n in (0, 7):
            value = x_in[n // 7, comp, :, lanes]
            row = edge_row(comp, n // 7, tile)
            sides = [edge_in[side, row : row + 1, :] for side in range(2)]
        else:
            value = local[comp, n, :, lanes]
            row = mid_row(comp, n, tile)
            sides = [mid_in[side, row : row + 1, :] for side in range(2)]
        where = lax.broadcasted_iota(jnp.int32, value.shape, 0)
        value = value + jnp.where(where == 0, sides[0], 0.0)
        return value + jnp.where(where == 7, sides[1], 0.0)

    def send_z():
        for side in range(2):
            tile, column = (tiles - 1, LANES - 1) if side == 0 else (0, 0)
            packed = jnp.zeros((8, LANES), jnp.float32)
            for comp in range(comps):
                for n in range(8):
                    value = xy_sum(comp, n, tile)[:, column : column + 1]
                    packed = jnp.where(lane == comp * 8 + n, value, packed)
            z_out[side] = packed
            when_do(target("gz", side), lambda: z_copy(side).start())

    def z_column(side, comp, n):
        at = comp * 8 + n
        return jnp.broadcast_to(z_in[side, :, at : at + 1], (8, LANES))

    def finish(which, first, last):
        for comp in range(comps):
            for n in which:
                parts = []
                for tile in range(first - 1, last + 1):
                    if tile < 0:
                        parts.append(z_column(0, comp, n))
                    elif tile == tiles:
                        parts.append(z_column(1, comp, n))
                    else:
                        parts.append(xy_sum(comp, n, tile))
                value = jnp.concatenate(parts, axis=1)
                width = value.shape[1]
                before = pltpu.roll(value, 1, 1)[:, LANES:-LANES]
                after = pltpu.roll(value, width - 1, 1)[:, LANES:-LANES]
                position = lax.broadcasted_iota(jnp.int32, before.shape, 1) % 8
                extra = jnp.where(position == 7, after, jnp.where(position == 0, before, 0.0))
                out[comp, n, :, first * LANES : last * LANES] = value[:, LANES:-LANES] + extra

    middle, ends = range(1, 7), (0, 7)
    def wait_z():
        take_both("gz", z_in, (), z_recv)

    finished = {middle: set(), ends: set()}
    arrived = {middle: set(), ends: set()}

    def finish_ready(which, with_z):
        have = arrived[which]

        def near(tile):
            return tile in have if 0 <= tile < tiles else with_z

        ready = [
            tile
            for tile in range(tiles)
            if tile not in finished[which] and all(near(tile + k) for k in (-1, 0, 1))
        ]
        while ready:
            first = last = ready.pop(0)
            while ready and ready[0] == last + 1 and last - first < GROUP - 1:
                last = ready.pop(0)
            finished[which].update(range(first, last + 1))
            finish(which, first, last + 1)

    greeted = sum(side[name].astype(jnp.int32) for name in names for side in (below, above))
    const_copies[2].wait()
    for at, c in enumerate(order):
        if at < 3:
            in_copies[at].wait()
        steps = [(c * CHUNK, CHUNK)]
        if at == 0:
            steps = [(c * CHUNK + k * LANES, LANES) for k in range(PER)]
        for start, size in steps:
            compute(start, size)
            if start == 0:
                pl.semaphore_wait(barrier, greeted)
            for side in range(2):
                when_do(target("gx", side), lambda: x_copy(side, start, size).start())
        if at == 1:
            send_mid(0)
        if at == 5:
            corners(0)
        if at == 6:
            send_mid(1)
    send_mid(2)
    send_mid(3)

    def take(which, g, wait, with_z):
        wait(g)
        arrived[which].update(groups[g])
        finish_ready(which, with_z)

    corners(1)
    wait_mid(0)
    wait_edge(0)
    send_z()
    arrived[middle].update(groups[0])
    arrived[ends].update(groups[0])
    corners(2)
    corners(3)
    take(middle, 1, wait_mid, False)
    take(middle, 2, wait_mid, False)
    wait_z()
    take(middle, 3, wait_mid, True)
    for g in range(1, 4):
        take(ends, g, wait_edge, True)

    for name, ref, semaphore in (
        ("gx", x_in, x_send),
        ("gy", mid_in, mid_send),
        ("gy", edge_in, edge_send),
        ("gz", z_in, z_send),
    ):
        take_both(name, ref, (), semaphore)


def local_part(sizes, nodal_scalar_values, geometry):
    comps, _, _, total = nodal_scalar_values.shape
    count = total // CHUNK
    _, groups = plan(total)
    mid_rows = offsets(groups, comps * 6)[1]
    edge_rows = offsets(groups, comps * 2)[1]
    matrices, scales = tables()
    f32 = jnp.float32
    dma = pltpu.SemaphoreType.DMA
    any_space = pl.BlockSpec(memory_space=pl.ANY)
    return pl.pallas_call(
        functools.partial(kernel, sizes),
        out_shape=pltpu.VMEM(nodal_scalar_values.shape, f32),
        in_specs=[any_space] * 4,
        out_specs=pl.BlockSpec(memory_space=pltpu.VMEM),
        scratch_shapes=[
            pltpu.VMEM(nodal_scalar_values.shape, f32),
            pltpu.VMEM(geometry.shape, f32),
            pltpu.VMEM(matrices.shape, jnp.bfloat16),
            pltpu.VMEM(scales.shape, f32),
            pltpu.VMEM(nodal_scalar_values.shape, f32),
            pltpu.VMEM((2, comps, 8, total), f32),
            pltpu.VMEM((2, mid_rows, LANES), f32),
            pltpu.VMEM((2, mid_rows, LANES), f32),
            pltpu.VMEM((2, edge_rows, LANES), f32),
            pltpu.VMEM((2, edge_rows, LANES), f32),
            pltpu.VMEM((2, 8, LANES), f32),
            pltpu.VMEM((2, 8, LANES), f32),
            dma((3,)),
            dma((3,)),
            dma,
            dma((count,)),
            dma,
            dma((len(groups),)),
            dma,
            dma((len(groups),)),
            dma,
            dma,
        ],
        compiler_params=pltpu.CompilerParams(collective_id=0, has_side_effects=True),
        name="poisson",
    )(nodal_scalar_values, geometry, jnp.asarray(matrices), jnp.asarray(scales))


def solution(mesh):
    return jax.shard_map(
        functools.partial(local_part, dict(mesh.shape)),
        mesh=mesh,
        in_specs=(P(None, "gx", "gy", "gz"), P(None, "gx", "gy", "gz")),
        out_specs=P(None, "gx", "gy", "gz"),
        check_vma=False,
    )
```

```python
import functools

import jax
import jax.numpy as jnp
import numpy as np
from jax import lax
from jax.experimental import pallas as pl
from jax.experimental.pallas import tpu as pltpu
from jax.sharding import PartitionSpec as P

interior_points = [
    -0.8717401485096066,
    -0.5917001814331423,
    -0.2092992179024789,
    0.2092992179024789,
    0.5917001814331423,
    0.8717401485096066,
]
MESH = pl.DeviceIdType.MESH
CHUNK = 256
LANES = 128
PER = CHUNK // LANES
GROUP = 4


def plan(total):
    count, tiles = total // CHUNK, total // LANES
    order = [0, count - 1] + list(range(1, count - 1))
    rest = [c * PER + k for c in order for k in range(PER)]
    return order, [rest[at : at + GROUP] for at in range(0, tiles, GROUP)]


def offsets(groups, rows):
    places, at = [], 0
    for group in groups:
        size = -(-len(group) * rows // 8) * 8
        places.append((at, size))
        at += size
    return places, at


def legendre_seven(point):
    previous = 1.0
    current = point
    for order in range(1, 7):
        following = ((2 * order + 1) * point * current - order * previous) / (order + 1)
        previous = current
        current = following
    return current


def gll_tables():
    degree = 7
    points = [-1.0] + interior_points + [1.0]
    values = [legendre_seven(point) for point in points]
    node_count = degree + 1
    weights = np.array([2.0 / (degree * (degree + 1) * value * value) for value in values])
    derivative = np.zeros((node_count, node_count))
    for row_index in range(node_count):
        for col_index in range(node_count):
            if row_index != col_index:
                derivative[row_index, col_index] = values[row_index] / (
                    values[col_index] * (points[row_index] - points[col_index])
                )
    derivative[0, 0] = -degree * (degree + 1) / 4.0
    derivative[node_count - 1, node_count - 1] = degree * (degree + 1) / 4.0
    return (derivative, weights)


def halves(table):
    table = np.asarray(table, np.float32)
    high = table.astype(jnp.bfloat16)
    low = (table - high.astype(np.float32)).astype(jnp.bfloat16)
    return high, low


def tables():
    derivative, weights = gll_tables()
    eye = np.eye(8)
    plane_weight = np.kron(weights, weights)
    forward_xy = np.concatenate([np.kron(derivative, eye), np.kron(eye, derivative)], axis=0)
    back_xy = np.concatenate([np.kron(derivative.T, eye), np.kron(eye, derivative.T)], axis=1)
    back_xy = back_xy * np.tile(plane_weight, 2)[None, :]
    forward_z = np.kron(np.eye(16), derivative.T)
    back_z = np.kron(np.eye(16), derivative)
    high, low = halves(forward_xy)
    forward_xy = np.concatenate([high, high, low, low], axis=1)
    high, low = halves(back_xy)
    back_xy = np.concatenate(
        [np.concatenate([high, high], axis=1), np.concatenate([low, low], axis=1)], axis=0
    )
    high, low = halves(forward_z)
    forward_z = np.concatenate([high, low], axis=1)
    high, low = halves(back_z)
    back_z = np.concatenate([high, low], axis=1)
    matrices = np.concatenate([forward_xy, back_xy, forward_z, back_z], axis=0)
    plane = np.repeat(plane_weight[:, None], LANES, axis=1)
    along = np.repeat(np.tile(weights, LANES // 8)[None, :], 8, axis=0)
    scales = np.concatenate([plane, along], axis=0).astype(np.float32)
    return matrices, scales


def split(value):
    high = value.astype(jnp.bfloat16)
    low = (value - high.astype(jnp.float32)).astype(jnp.bfloat16)
    return high, low


def product(left, right):
    return jnp.dot(left, right, preferred_element_type=jnp.float32)


def along_lanes(high, low, table):
    pieces = []
    for start in range(0, high.shape[1], LANES):
        both = jnp.concatenate(
            [high[:, start : start + LANES], low[:, start : start + LANES]], axis=1
        )
        twice = product(both, table)
        pieces.append(twice[:, :LANES] + twice[:, LANES:])
    return jnp.concatenate(pieces, axis=1)


def kernel(
    sizes,
    u_hbm,
    geo_hbm,
    mat_hbm,
    scale_hbm,
    out,
    u,
    geo,
    mat,
    scale,
    local,
    x_in,
    mid_out,
    mid_in,
    edge_out,
    edge_in,
    z_out,
    z_in,
    in_sem,
    const_sem,
    x_send,
    x_recv,
    mid_send,
    mid_recv,
    edge_send,
    edge_recv,
    z_send,
    z_recv,
):
    comps, _, _, total = u.shape
    tiles = total // LANES
    order, groups = plan(total)
    mid_place, _ = offsets(groups, comps * 6)
    edge_place, _ = offsets(groups, comps * 2)
    group_of = {tile: (g, k) for g, group in enumerate(groups) for k, tile in enumerate(group)}
    names = ("gx", "gy", "gz")
    place = {name: lax.axis_index(name) for name in names}
    below = {name: place[name] > 0 for name in names}
    above = {name: place[name] < sizes[name] - 1 for name in names}

    barrier = pltpu.get_barrier_semaphore()
    for name in names:
        for there, by in ((below[name], -1), (above[name], 1)):

            @pl.when(there)
            def _(name=name, by=by):
                pl.semaphore_signal(
                    barrier, inc=1, device_id={name: place[name] + by}, device_id_type=MESH
                )

    def in_copy(at, first, last):
        span = pl.ds(first * CHUNK, (last - first) * CHUNK)
        return pltpu.make_async_copy(
            u_hbm.at[:, :, :, span], u.at[:, :, :, span], in_sem.at[at]
        )

    count = total // CHUNK
    in_copies = [in_copy(0, 0, 1), in_copy(1, count - 1, count), in_copy(2, 1, count - 1)]
    const_copies = [
        pltpu.make_async_copy(geo_hbm, geo, const_sem.at[0]),
        pltpu.make_async_copy(scale_hbm, scale, const_sem.at[1]),
        pltpu.make_async_copy(mat_hbm, mat, const_sem.at[2]),
    ]
    in_copies[0].start()
    for copy in const_copies:
        copy.start()

    for copy in in_copies[1:]:
        copy.start()

    def target(name, side):
        return above[name] if side == 0 else below[name]

    def source(name, side):
        return below[name] if side == 0 else above[name]

    def when_do(condition, act):
        @pl.when(condition)
        def _():
            act()

    for side in range(2):

        @pl.when(jnp.logical_not(source("gx", side)))
        def _(side=side):
            x_in[side] = jnp.zeros(x_in.shape[1:], jnp.float32)

        @pl.when(jnp.logical_not(source("gy", side)))
        def _(side=side):
            mid_in[side] = jnp.zeros(mid_in.shape[1:], jnp.float32)
            edge_in[side] = jnp.zeros(edge_in.shape[1:], jnp.float32)

        @pl.when(jnp.logical_not(source("gz", side)))
        def _(side=side):
            z_in[side] = jnp.zeros(z_in.shape[1:], jnp.float32)

    def neighbour(name, side):
        return {name: place[name] + (1 if side == 0 else -1)}

    def x_copy(side, c):
        span = pl.ds(c * CHUNK, CHUNK)
        return pltpu.make_async_remote_copy(
            local.at[:, 7 if side == 0 else 0, :, span],
            x_in.at[side, :, :, span],
            x_send,
            x_recv.at[c],
            device_id=neighbour("gx", side),
            device_id_type=MESH,
        )

    def mid_copy(side, g):
        span = pl.ds(*mid_place[g])
        return pltpu.make_async_remote_copy(
            mid_out.at[side, span],
            mid_in.at[side, span],
            mid_send,
            mid_recv.at[g],
            device_id=neighbour("gy", side),
            device_id_type=MESH,
        )

    def edge_copy(side, g):
        span = pl.ds(*edge_place[g])
        return pltpu.make_async_remote_copy(
            edge_out.at[side, span],
            edge_in.at[side, span],
            edge_send,
            edge_recv.at[g],
            device_id=neighbour("gy", side),
            device_id_type=MESH,
        )

    def z_copy(side):
        return pltpu.make_async_remote_copy(
            z_out.at[side],
            z_in.at[side],
            z_send,
            z_recv,
            device_id=neighbour("gz", side),
            device_id_type=MESH,
        )

    def take_both(name, ref, part, semaphore):
        both = jnp.logical_and(below[name], above[name])
        one = jnp.logical_xor(below[name], above[name])
        for condition, sides in ((both, 2), (one, 1)):
            piece = ref.at[(pl.ds(0, sides),) + part]
            when_do(condition, lambda: pltpu.make_async_copy(piece, piece, semaphore).wait())

    def mid_row(comp, n, tile):
        g, k = group_of[tile]
        return mid_place[g][0] + k * comps * 6 + comp * 6 + n - 1

    def edge_row(comp, end, tile):
        g, k = group_of[tile]
        return edge_place[g][0] + k * comps * 2 + comp * 2 + end

    for copy in const_copies[:2]:
        copy.wait()
    rows = jnp.concatenate(
        [geo[k, 0] for k in range(6)] + [jnp.zeros((2, geo.shape[-1]), jnp.float32)], axis=0
    )
    lane = lax.broadcasted_iota(jnp.int32, (8, LANES), 1)

    def metric_of(tile):
        first = tile * (LANES // 8)
        block = rows[:, first // LANES * LANES : first // LANES * LANES + LANES]
        spread = jnp.take_along_axis(block, lane // 8 + first % LANES, axis=1)
        return spread * scale[64:72, :]

    def compute(start, size):
        lanes = slice(start, start + size)
        metric = jnp.concatenate(
            [metric_of(start // LANES + k) for k in range(size // LANES)], axis=1
        )
        g00, g11, g22, g01, g02, g12 = [metric[k : k + 1] for k in range(6)]
        forward_xy, back_xy = mat[0:128, :], mat[128:256, :]
        forward_z = jnp.concatenate([mat[256:384, :]] * 2, axis=0)
        back_z = jnp.concatenate([mat[384:512, :]] * 2, axis=0)
        for comp in range(comps):
            field = u[comp, :, :, lanes].reshape(64, size)
            high, low = split(field)
            both = product(forward_xy, jnp.concatenate([high, low, high, low], axis=0))
            grad_x, grad_y = both[:64], both[64:]
            grad_z = along_lanes(high, low, forward_z)
            flux_x = g00 * grad_x + g01 * grad_y + g02 * grad_z
            flux_y = g01 * grad_x + g11 * grad_y + g12 * grad_z
            flux_z = g02 * grad_x + g12 * grad_y + g22 * grad_z
            x_high, x_low = split(flux_x)
            y_high, y_low = split(flux_y)
            z_high, z_low = split(flux_z)
            twice = product(back_xy, jnp.concatenate([x_high, y_high, x_low, y_low], axis=0))
            terms = twice[:64] + twice[64:]
            weight = jnp.concatenate([scale[0:64, :]] * (size // LANES), axis=1)
            terms = terms + weight * along_lanes(z_high, z_low, back_z)
            terms = terms.reshape(8, 8, size)
            local[comp, :, :, lanes] = terms
            for n in range(1, 7):
                for k in range(size // LANES):
                    row = mid_row(comp, n, start // LANES + k)
                    part = slice(k * LANES, (k + 1) * LANES)
                    mid_out[0, row : row + 1, :] = terms[n, 7:8, part]
                    mid_out[1, row : row + 1, :] = terms[n, 0:1, part]

    x_here = set()

    def wait_x(c):
        if c not in x_here:
            x_here.add(c)
            span = pl.ds(c * CHUNK, CHUNK)
            take_both("gx", x_in, (slice(None), slice(None), span), x_recv.at[c])

    def corners(g):
        for tile in groups[g]:
            wait_x(tile // PER)
        for comp in range(comps):
            for end in range(2):
                for tile in groups[g]:
                    lanes = slice(tile * LANES, (tile + 1) * LANES)
                    value = local[comp, 7 * end, :, lanes] + x_in[end, comp, :, lanes]
                    x_in[end, comp, :, lanes] = value
                    row = edge_row(comp, end, tile)
                    edge_out[0, row : row + 1, :] = value[7:8]
                    edge_out[1, row : row + 1, :] = value[0:1]
        for side in range(2):
            when_do(target("gy", side), lambda: edge_copy(side, g).start())

    def send_mid(g):
        for side in range(2):
            when_do(target("gy", side), lambda: mid_copy(side, g).start())

    def wait_mid(g):
        take_both("gy", mid_in, (pl.ds(*mid_place[g]),), mid_recv.at[g])

    def wait_edge(g):
        take_both("gy", edge_in, (pl.ds(*edge_place[g]),), edge_recv.at[g])

    def xy_sum(comp, n, tile):
        lanes = slice(tile * LANES, (tile + 1) * LANES)
        if n in (0, 7):
            value = x_in[n // 7, comp, :, lanes]
            row = edge_row(comp, n // 7, tile)
            sides = [edge_in[side, row : row + 1, :] for side in range(2)]
        else:
            value = local[comp, n, :, lanes]
            row = mid_row(comp, n, tile)
            sides = [mid_in[side, row : row + 1, :] for side in range(2)]
        where = lax.broadcasted_iota(jnp.int32, value.shape, 0)
        value = value + jnp.where(where == 0, sides[0], 0.0)
        return value + jnp.where(where == 7, sides[1], 0.0)

    def send_z():
        for side in range(2):
            tile, column = (tiles - 1, LANES - 1) if side == 0 else (0, 0)
            packed = jnp.zeros((8, LANES), jnp.float32)
            for comp in range(comps):
                for n in range(8):
                    value = xy_sum(comp, n, tile)[:, column : column + 1]
                    packed = jnp.where(lane == comp * 8 + n, value, packed)
            z_out[side] = packed
            when_do(target("gz", side), lambda: z_copy(side).start())

    def z_column(side, comp, n):
        at = comp * 8 + n
        return jnp.broadcast_to(z_in[side, :, at : at + 1], (8, LANES))

    def finish(which, first, last):
        for comp in range(comps):
            for n in which:
                parts = []
                for tile in range(first - 1, last + 1):
                    if tile < 0:
                        parts.append(z_column(0, comp, n))
                    elif tile == tiles:
                        parts.append(z_column(1, comp, n))
                    else:
                        parts.append(xy_sum(comp, n, tile))
                value = jnp.concatenate(parts, axis=1)
                width = value.shape[1]
                before = pltpu.roll(value, 1, 1)[:, LANES:-LANES]
                after = pltpu.roll(value, width - 1, 1)[:, LANES:-LANES]
                position = lax.broadcasted_iota(jnp.int32, before.shape, 1) % 8
                extra = jnp.where(position == 7, after, jnp.where(position == 0, before, 0.0))
                out[comp, n, :, first * LANES : last * LANES] = value[:, LANES:-LANES] + extra

    middle, ends = range(1, 7), (0, 7)
    def wait_z():
        take_both("gz", z_in, (), z_recv)

    finished = {middle: set(), ends: set()}
    arrived = {middle: set(), ends: set()}

    def finish_ready(which, with_z):
        have = arrived[which]

        def near(tile):
            return tile in have if 0 <= tile < tiles else with_z

        ready = [
            tile
            for tile in range(tiles)
            if tile not in finished[which] and all(near(tile + k) for k in (-1, 0, 1))
        ]
        while ready:
            first = last = ready.pop(0)
            while ready and ready[0] == last + 1 and last - first < GROUP - 1:
                last = ready.pop(0)
            finished[which].update(range(first, last + 1))
            finish(which, first, last + 1)

    greeted = sum(side[name].astype(jnp.int32) for name in names for side in (below, above))
    const_copies[2].wait()
    for at, c in enumerate(order):
        if at < 3:
            in_copies[at].wait()
        compute(c * CHUNK, CHUNK)
        if at == 0:
            pl.semaphore_wait(barrier, greeted)
        for side in range(2):
            when_do(target("gx", side), lambda: x_copy(side, c).start())
        if at == 1:
            send_mid(0)
        if at == 5:
            corners(0)
        if at == 6:
            send_mid(1)
    send_mid(2)
    send_mid(3)

    def take(which, g, wait, with_z):
        wait(g)
        arrived[which].update(groups[g])
        finish_ready(which, with_z)

    corners(1)
    wait_mid(0)
    wait_edge(0)
    send_z()
    arrived[middle].update(groups[0])
    arrived[ends].update(groups[0])
    corners(2)
    corners(3)
    take(middle, 1, wait_mid, False)
    take(middle, 2, wait_mid, False)
    wait_z()
    take(middle, 3, wait_mid, True)
    for g in range(1, 4):
        take(ends, g, wait_edge, True)

    for name, ref, semaphore in (
        ("gx", x_in, x_send),
        ("gy", mid_in, mid_send),
        ("gy", edge_in, edge_send),
        ("gz", z_in, z_send),
    ):
        take_both(name, ref, (), semaphore)


def local_part(sizes, nodal_scalar_values, geometry):
    comps, _, _, total = nodal_scalar_values.shape
    count = total // CHUNK
    _, groups = plan(total)
    mid_rows = offsets(groups, comps * 6)[1]
    edge_rows = offsets(groups, comps * 2)[1]
    matrices, scales = tables()
    f32 = jnp.float32
    dma = pltpu.SemaphoreType.DMA
    any_space = pl.BlockSpec(memory_space=pl.ANY)
    return pl.pallas_call(
        functools.partial(kernel, sizes),
        out_shape=pltpu.VMEM(nodal_scalar_values.shape, f32),
        in_specs=[any_space] * 4,
        out_specs=pl.BlockSpec(memory_space=pltpu.VMEM),
        scratch_shapes=[
            pltpu.VMEM(nodal_scalar_values.shape, f32),
            pltpu.VMEM(geometry.shape, f32),
            pltpu.VMEM(matrices.shape, jnp.bfloat16),
            pltpu.VMEM(scales.shape, f32),
            pltpu.VMEM(nodal_scalar_values.shape, f32),
            pltpu.VMEM((2, comps, 8, total), f32),
            pltpu.VMEM((2, mid_rows, LANES), f32),
            pltpu.VMEM((2, mid_rows, LANES), f32),
            pltpu.VMEM((2, edge_rows, LANES), f32),
            pltpu.VMEM((2, edge_rows, LANES), f32),
            pltpu.VMEM((2, 8, LANES), f32),
            pltpu.VMEM((2, 8, LANES), f32),
            dma((3,)),
            dma((3,)),
            dma,
            dma((count,)),
            dma,
            dma((len(groups),)),
            dma,
            dma((len(groups),)),
            dma,
            dma,
        ],
        compiler_params=pltpu.CompilerParams(collective_id=0, has_side_effects=True),
        name="poisson",
    )(nodal_scalar_values, geometry, jnp.asarray(matrices), jnp.asarray(scales))


def solution(mesh):
    return jax.shard_map(
        functools.partial(local_part, dict(mesh.shape)),
        mesh=mesh,
        in_specs=(P(None, "gx", "gy", "gz"), P(None, "gx", "gy", "gz")),
        out_specs=P(None, "gx", "gy", "gz"),
        check_vma=False,
    )
```

```python
import functools

import jax
import jax.numpy as jnp
import numpy as np
from jax import lax
from jax.experimental import pallas as pl
from jax.experimental.pallas import tpu as pltpu
from jax.sharding import PartitionSpec as P

interior_points = [
    -0.8717401485096066,
    -0.5917001814331423,
    -0.2092992179024789,
    0.2092992179024789,
    0.5917001814331423,
    0.8717401485096066,
]
MESH = pl.DeviceIdType.MESH
CHUNK = 256
LANES = 128
PER = CHUNK // LANES
GROUP = 4
LINES = 8


def plan(total):
    count, tiles = total // CHUNK, total // LANES
    order = [1, 2, 0, count - 1] + list(range(3, count - 1))
    late = list(range(1, count - 1)) + [0, count - 1]
    rest = [c * PER + k for c in late for k in range(PER)]
    return order, [rest[at : at + GROUP] for at in range(0, tiles, GROUP)]


def offsets(groups, rows):
    places, at = [], 0
    for group in groups:
        size = -(-len(group) * rows // 8) * 8
        places.append((at, size))
        at += size
    return places, at


def legendre_seven(point):
    previous = 1.0
    current = point
    for order in range(1, 7):
        following = ((2 * order + 1) * point * current - order * previous) / (order + 1)
        previous = current
        current = following
    return current


def gll_tables():
    degree = 7
    points = [-1.0] + interior_points + [1.0]
    values = [legendre_seven(point) for point in points]
    node_count = degree + 1
    weights = np.array([2.0 / (degree * (degree + 1) * value * value) for value in values])
    derivative = np.zeros((node_count, node_count))
    for row_index in range(node_count):
        for col_index in range(node_count):
            if row_index != col_index:
                derivative[row_index, col_index] = values[row_index] / (
                    values[col_index] * (points[row_index] - points[col_index])
                )
    derivative[0, 0] = -degree * (degree + 1) / 4.0
    derivative[node_count - 1, node_count - 1] = degree * (degree + 1) / 4.0
    return (derivative, weights)


def halves(table):
    table = np.asarray(table, np.float32)
    high = table.astype(jnp.bfloat16)
    low = (table - high.astype(np.float32)).astype(jnp.bfloat16)
    return high, low


def tables():
    derivative, weights = gll_tables()
    eye = np.eye(8)
    plane_weight = np.kron(weights, weights)
    forward_xy = np.concatenate([np.kron(derivative, eye), np.kron(eye, derivative)], axis=0)
    back_xy = np.concatenate([np.kron(derivative.T, eye), np.kron(eye, derivative.T)], axis=1)
    back_xy = back_xy * np.tile(plane_weight, 2)[None, :]
    forward_z = np.kron(np.eye(16), derivative.T)
    back_z = np.kron(np.eye(16), derivative)
    high, low = halves(forward_xy)
    forward_xy = np.concatenate([high, high, low, low], axis=1)
    high, low = halves(back_xy)
    back_xy = np.concatenate(
        [np.concatenate([high, high], axis=1), np.concatenate([low, low], axis=1)], axis=0
    )
    high, low = halves(forward_z)
    forward_z = np.concatenate([high, low], axis=1)
    high, low = halves(back_z)
    back_z = np.concatenate([high, low], axis=1)
    matrices = np.concatenate([forward_xy, back_xy, forward_z, back_z], axis=0)
    plane = np.repeat(plane_weight[:, None], LANES, axis=1)
    along = np.repeat(np.tile(weights, LANES // 8)[None, :], 8, axis=0)
    scales = np.concatenate([plane, along], axis=0).astype(np.float32)
    return matrices, scales


def split(value):
    high = value.astype(jnp.bfloat16)
    low = (value - high.astype(jnp.float32)).astype(jnp.bfloat16)
    return high, low


def product(left, right):
    return jnp.dot(left, right, preferred_element_type=jnp.float32)


def along_lanes(high, low, table):
    pieces = []
    for start in range(0, high.shape[1], LANES):
        both = jnp.concatenate(
            [high[:, start : start + LANES], low[:, start : start + LANES]], axis=1
        )
        twice = product(both, table)
        pieces.append(twice[:, :LANES] + twice[:, LANES:])
    return jnp.concatenate(pieces, axis=1)


def kernel(
    sizes,
    u_hbm,
    geo_hbm,
    mat_hbm,
    scale_hbm,
    out,
    u,
    geo,
    mat,
    scale,
    local,
    x_in,
    mid_out,
    mid_in,
    leaf_out,
    hub_own,
    hub_in,
    hub_out,
    hub_x,
    line_sum,
    z_out,
    z_in,
    in_sem,
    const_sem,
    x_send,
    x_recv,
    mid_send,
    mid_recv,
    leaf_send,
    leaf_recv,
    hub_send,
    hub_recv,
    sum_send,
    sum_recv,
    z_send,
    z_recv,
):
    comps, _, _, total = u.shape
    tiles = total // LANES
    order, groups = plan(total)
    mid_place, _ = offsets(groups, comps * 6)
    line_tiles = [tile for group in groups for tile in group]
    line_at = {tile: k for k, tile in enumerate(line_tiles)}
    line_rows = LINES * comps
    group_of = {tile: (g, k) for g, group in enumerate(groups) for k, tile in enumerate(group)}
    names = ("gx", "gy", "gz")
    place = {name: lax.axis_index(name) for name in names}
    below = {name: place[name] > 0 for name in names}
    above = {name: place[name] < sizes[name] - 1 for name in names}

    def target(name, side):
        return above[name] if side == 0 else below[name]

    def source(name, side):
        return below[name] if side == 0 else above[name]

    def when_do(condition, act):
        @pl.when(condition)
        def _():
            act()

    upper = lax.rem(place["gy"], 2)
    lower = 1 - upper
    inside = jnp.logical_and(below["gy"], above["gy"])
    facing = place["gx"] + upper - lower
    paired = jnp.logical_and(facing >= 0, facing < sizes["gx"])

    def across(side):
        return {"gx": facing, "gy": place["gy"] + (1 if side else -1)}

    barrier = pltpu.get_barrier_semaphore()
    for name in names:
        for there, by in ((below[name], -1), (above[name], 1)):

            @pl.when(there)
            def _(name=name, by=by):
                pl.semaphore_signal(
                    barrier, inc=1, device_id={name: place[name] + by}, device_id_type=MESH
                )

    greeted = sum(side[name].astype(jnp.int32) for name in names for side in (below, above))
    for side in range(2):
        there = jnp.logical_and(paired, source("gy", side))
        greeted = greeted + there.astype(jnp.int32)

        @pl.when(there)
        def _(side=side):
            pl.semaphore_signal(barrier, inc=1, device_id=across(side), device_id_type=MESH)

    def in_copy(at, first, last):
        span = pl.ds(first * CHUNK, (last - first) * CHUNK)
        return pltpu.make_async_copy(
            u_hbm.at[:, :, :, span], u.at[:, :, :, span], in_sem.at[at]
        )

    count = total // CHUNK
    in_copies = [
        in_copy(0, 1, 2),
        in_copy(1, 2, count - 1),
        in_copy(2, 0, 1),
        in_copy(3, count - 1, count),
    ]
    const_copies = [
        pltpu.make_async_copy(geo_hbm, geo, const_sem.at[0]),
        pltpu.make_async_copy(scale_hbm, scale, const_sem.at[1]),
        pltpu.make_async_copy(mat_hbm, mat, const_sem.at[2]),
    ]
    in_copies[0].start()
    for copy in const_copies:
        copy.start()

    for copy in in_copies[1:]:
        copy.start()

    for side in range(2):

        @pl.when(jnp.logical_not(source("gx", side)))
        def _(side=side):
            x_in[side] = jnp.zeros(x_in.shape[1:], jnp.float32)

        @pl.when(jnp.logical_not(source("gy", side)))
        def _(side=side):
            mid_in[side] = jnp.zeros(mid_in.shape[1:], jnp.float32)

        @pl.when(jnp.logical_not(source("gz", side)))
        def _(side=side):
            z_in[side] = jnp.zeros(z_in.shape[1:], jnp.float32)

    @pl.when(jnp.logical_not(paired))
    def _():
        hub_x[...] = jnp.zeros(hub_x.shape, jnp.float32)

    def neighbour(name, side):
        return {name: place[name] + (1 if side == 0 else -1)}

    def x_copy(side, c, rows):
        span = pl.ds(c * CHUNK, CHUNK)
        return pltpu.make_async_remote_copy(
            local.at[:, 7 if side == 0 else 0, rows, span],
            x_in.at[side, :, rows, span],
            x_send,
            x_recv.at[c],
            device_id=neighbour("gx", side),
            device_id_type=MESH,
        )

    def mid_copy(side, g):
        span = pl.ds(*mid_place[g])
        return pltpu.make_async_remote_copy(
            mid_out.at[side, span],
            mid_in.at[side, span],
            mid_send,
            mid_recv.at[g],
            device_id=neighbour("gy", side),
            device_id_type=MESH,
        )

    def line_span(h):
        return pl.ds(h * line_rows, line_rows)

    def leaf_copy(side, h):
        return pltpu.make_async_remote_copy(
            leaf_out.at[side, line_span(h)],
            hub_in.at[side, line_span(h)],
            leaf_send,
            leaf_recv.at[h],
            device_id=neighbour("gy", side),
            device_id_type=MESH,
        )

    def hub_copy(side, h):
        return pltpu.make_async_remote_copy(
            hub_out.at[side, line_span(h)],
            hub_x.at[1 - side, line_span(h)],
            hub_send,
            hub_recv.at[h],
            device_id=across(side),
            device_id_type=MESH,
        )

    def sum_copy(side, h):
        return pltpu.make_async_remote_copy(
            line_sum.at[upper, side, line_span(h)],
            line_sum.at[upper, 1 - side, line_span(h)],
            sum_send,
            sum_recv.at[h],
            device_id={"gy": place["gy"] + (1 if side else -1)},
            device_id_type=MESH,
        )

    def z_copy(side):
        return pltpu.make_async_remote_copy(
            z_out.at[side],
            z_in.at[side],
            z_send,
            z_recv,
            device_id=neighbour("gz", side),
            device_id_type=MESH,
        )

    every = slice(None)
    within = pl.ds(1, 6)

    def take_both(name, piece, semaphore, also=None):
        both = jnp.logical_and(below[name], above[name])
        one = jnp.logical_xor(below[name], above[name])
        for condition, sides in ((both, 2), (one, 1)):
            ref = piece(pl.ds(0, sides))
            if also is not None:
                condition = jnp.logical_and(condition, also)
            when_do(condition, lambda: pltpu.make_async_copy(ref, ref, semaphore).wait())

    def take_x(span, semaphore):
        for rows, also in ((within, inside), (every, jnp.logical_not(inside))):
            take_both("gx", lambda sides: x_in.at[sides, :, rows, span], semaphore, also)

    def way(side, near):
        near_side = (upper if side else lower) > 0
        return near_side if near else jnp.logical_not(near_side)

    def send_x(c, near=None):
        for side in range(2):
            there = target("gx", side)
            if near is not None:
                there = jnp.logical_and(there, way(side, near))
            for rows, also in ((within, inside), (every, jnp.logical_not(inside))):
                when_do(jnp.logical_and(there, also), lambda: x_copy(side, c, rows).start())

    def mid_row(comp, n, tile):
        g, k = group_of[tile]
        return mid_place[g][0] + k * comps * 6 + comp * 6 + n - 1

    def line_row(comp, tile):
        return line_at[tile] * comps + comp

    for copy in const_copies[:2]:
        copy.wait()
    rows = jnp.concatenate(
        [geo[k, 0] for k in range(6)] + [jnp.zeros((2, geo.shape[-1]), jnp.float32)], axis=0
    )
    lane = lax.broadcasted_iota(jnp.int32, (8, LANES), 1)

    def metric_of(tile):
        first = tile * (LANES // 8)
        block = rows[:, first // LANES * LANES : first // LANES * LANES + LANES]
        spread = jnp.take_along_axis(block, lane // 8 + first % LANES, axis=1)
        return spread * scale[64:72, :]

    def compute(start, size):
        lanes = slice(start, start + size)
        metric = jnp.concatenate(
            [metric_of(start // LANES + k) for k in range(size // LANES)], axis=1
        )
        g00, g11, g22, g01, g02, g12 = [metric[k : k + 1] for k in range(6)]
        forward_xy, back_xy = mat[0:128, :], mat[128:256, :]
        forward_z = jnp.concatenate([mat[256:384, :]] * 2, axis=0)
        back_z = jnp.concatenate([mat[384:512, :]] * 2, axis=0)
        pieces = range(0, size, LANES)

        def along_all(pairs, table):
            blocks = [
                jnp.concatenate([part[:, at : at + LANES] for part in pair], axis=1)
                for pair in pairs
                for at in pieces
            ]
            twice = product(jnp.concatenate(blocks, axis=0), table)
            sums = twice[:, :LANES] + twice[:, LANES:]
            sums = [sums[64 * k : 64 * (k + 1)] for k in range(len(blocks))]
            count = len(pieces)
            return [
                jnp.concatenate(sums[k * count : (k + 1) * count], axis=1)
                for k in range(len(pairs))
            ]

        fields = [split(u[comp, :, :, lanes].reshape(64, size)) for comp in range(comps)]
        grads_z = along_all(fields, forward_z)
        partial, fluxes_z = [], []
        for comp in range(comps):
            high, low = fields[comp]
            both = product(forward_xy, jnp.concatenate([high, low, high, low], axis=0))
            grad_x, grad_y, grad_z = both[:64], both[64:], grads_z[comp]
            flux_x = g00 * grad_x + g01 * grad_y + g02 * grad_z
            flux_y = g01 * grad_x + g11 * grad_y + g12 * grad_z
            flux_z = g02 * grad_x + g12 * grad_y + g22 * grad_z
            x_high, x_low = split(flux_x)
            y_high, y_low = split(flux_y)
            fluxes_z.append(split(flux_z))
            twice = product(back_xy, jnp.concatenate([x_high, y_high, x_low, y_low], axis=0))
            partial.append(twice[:64] + twice[64:])
        weight = jnp.concatenate([scale[0:64, :]] * (size // LANES), axis=1)
        terms_z = along_all(fluxes_z, back_z)
        for comp in range(comps):
            terms = partial[comp] + weight * terms_z[comp]
            terms = terms.reshape(8, 8, size)
            local[comp, :, :, lanes] = terms
            for k in range(size // LANES):
                tile = start // LANES + k
                if tile in (0, tiles - 1):
                    continue
                part = slice(k * LANES, (k + 1) * LANES)
                for n in range(1, 7):
                    put_mid(comp, n, tile, terms[n, :, part])

    def put_mid(comp, n, tile, value):
        row = mid_row(comp, n, tile)
        mid_out[0, row : row + 1, :] = value[7:8]
        mid_out[1, row : row + 1, :] = value[0:1]

    x_here = set()

    def wait_x(tile):
        c = tile // PER
        if c not in x_here:
            x_here.add(c)
            take_x(pl.ds(c * CHUNK, CHUNK), x_recv.at[c])

    def send_leaf(h):
        for tile in line_tiles[h * LINES : (h + 1) * LINES]:
            lanes = slice(tile * LANES, (tile + 1) * LANES)
            for comp in range(comps):
                row = line_row(comp, tile)
                leaf = local[comp, 7 * lower, :, lanes]
                leaf_out[0, row : row + 1, :] = leaf[7:8]
                leaf_out[1, row : row + 1, :] = leaf[0:1]
                own = local[comp, 7 * upper, :, lanes]
                hub_own[0, row : row + 1, :] = own[0:1]
                hub_own[1, row : row + 1, :] = own[7:8]
        for side in range(2):
            when_do(target("gy", side), lambda: leaf_copy(side, h).start())

    def send_hub(h):
        span = line_span(h)
        take_both("gy", lambda sides: hub_in.at[sides, span], leaf_recv.at[h])
        for side in range(2):
            hub_out[side, span] = hub_own[side, span] + hub_in[side, span]
            there = jnp.logical_and(paired, source("gy", side))
            when_do(there, lambda: hub_copy(side, h).start())

    def send_sum(h):
        span = line_span(h)
        take_both("gy", lambda sides: hub_x.at[sides, span], hub_recv.at[h], paired)
        for side in range(2):
            line_sum[upper, side, span] = hub_out[side, span] + hub_x[side, span]
            when_do(source("gy", side), lambda: sum_copy(side, h).start())

    def wait_sum(h):
        take_both("gy", lambda sides: line_sum.at[lower, sides, line_span(h)], sum_recv.at[h])

    def send_mid(g, near):
        for side in range(2):
            there = jnp.logical_and(target("gy", side), way(side, near))
            when_do(there, lambda: mid_copy(side, g).start())

    def wait_mid(g):
        take_both("gy", lambda sides: mid_in.at[sides, pl.ds(*mid_place[g])], mid_recv.at[g])

    def xy_sum(comp, n, tile):
        lanes = slice(tile * LANES, (tile + 1) * LANES)
        where = lax.broadcasted_iota(jnp.int32, (8, LANES), 0)
        if n in (0, 7):
            value = local[comp, n, :, lanes] + x_in[n // 7, comp, :, lanes]
            row = line_row(comp, tile)
            first, last = [line_sum[n // 7, side, row : row + 1, :] for side in range(2)]
            value = jnp.where(where == first_line, first, value)
            return jnp.where(where == last_line, last, value)
        value = local[comp, n, :, lanes]
        row = mid_row(comp, n, tile)
        sides = [mid_in[side, row : row + 1, :] for side in range(2)]
        value = value + jnp.where(where == 0, sides[0], 0.0)
        return value + jnp.where(where == 7, sides[1], 0.0)

    first_line = jnp.where(below["gy"], 0, 8)
    last_line = jnp.where(above["gy"], 7, 8)

    def outer(side):
        return (0, 0) if side else (tiles - 1, LANES - 1)

    def send_z():
        for side in range(2):
            tile, column = outer(side)
            lanes = slice(tile * LANES, (tile + 1) * LANES)
            packed = jnp.zeros((8, LANES), jnp.float32)
            for comp in range(comps):
                for n in range(8):
                    value = local[comp, n, :, lanes][:, column : column + 1]
                    packed = jnp.where(lane == comp * 8 + n, value, packed)
            z_out[side] = packed
            when_do(target("gz", side), lambda: z_copy(side).start())

    def add_z():
        take_both("gz", lambda sides: z_in.at[sides], z_recv)
        for side in range(2):
            tile, column = outer(1 - side)
            lanes = slice(tile * LANES, (tile + 1) * LANES)
            arrived_z = z_in[side]
            for comp in range(comps):
                for n in range(8):
                    at = comp * 8 + n
                    extra = jnp.where(lane == column, arrived_z[:, at : at + 1], 0.0)
                    value = local[comp, n, :, lanes] + extra
                    local[comp, n, :, lanes] = value
                    if 0 < n < 7:
                        put_mid(comp, n, tile, value)

    def finish(which, first, last):
        for comp in range(comps):
            for n in which:
                parts = []
                for tile in range(first - 1, last + 1):
                    if 0 <= tile < tiles:
                        parts.append(xy_sum(comp, n, tile))
                    else:
                        parts.append(jnp.zeros((8, LANES), jnp.float32))
                value = jnp.concatenate(parts, axis=1)
                width = value.shape[1]
                before = pltpu.roll(value, 1, 1)[:, LANES:-LANES]
                after = pltpu.roll(value, width - 1, 1)[:, LANES:-LANES]
                position = lax.broadcasted_iota(jnp.int32, before.shape, 1) % 8
                extra = jnp.where(position == 7, after, jnp.where(position == 0, before, 0.0))
                out[comp, n, :, first * LANES : last * LANES] = value[:, LANES:-LANES] + extra

    middle, ends = range(1, 7), (0, 7)
    finished = {middle: set(), ends: set()}
    arrived = {middle: set(), ends: set()}

    def finish_ready(which):
        have = arrived[which]

        def near(tile):
            return tile in have or not 0 <= tile < tiles

        ready = [
            tile
            for tile in range(tiles)
            if tile not in finished[which] and all(near(tile + k) for k in (-1, 0, 1))
        ]
        while ready:
            first = last = ready.pop(0)
            while ready and ready[0] == last + 1 and last - first < GROUP - 1:
                last = ready.pop(0)
            finished[which].update(range(first, last + 1))
            finish(which, first, last + 1)

    const_copies[2].wait()
    for at, c in enumerate(order):
        if at < 4:
            in_copies[at].wait()
        compute(c * CHUNK, CHUNK)
        if at == 0:
            pl.semaphore_wait(barrier, greeted)
        if at == 3:
            send_z()
        if at == 5:
            send_leaf(0)
        if 0 < c < count - 2:
            send_x(c)
        if at == 1:
            send_mid(0, True)
    add_z()
    send_leaf(1)
    last = (count - 2, 0, count - 1)
    for c in last:
        send_x(c, True)

    def take_mid(g):
        wait_mid(g)
        arrived[middle].update(groups[g])
        finish_ready(middle)

    def take_ends(h):
        wait_sum(h)
        now = line_tiles[h * LINES : (h + 1) * LINES]
        for tile in now:
            wait_x(tile)
        arrived[ends].update(now)
        finish_ready(ends)

    for g in (1, 2, 3):
        send_mid(g, True)
    send_hub(0)
    send_hub(1)
    for c in last:
        send_x(c, False)
    send_mid(0, False)
    send_mid(1, False)
    send_sum(0)
    send_mid(2, False)
    send_sum(1)
    send_mid(3, False)
    take_mid(0)
    take_ends(0)
    take_mid(1)
    take_mid(2)
    take_ends(1)
    take_mid(3)

    take_x(every, x_send)
    for piece, semaphore, also in (
        (lambda sides: mid_in.at[sides], mid_send, None),
        (lambda sides: hub_in.at[sides], leaf_send, None),
        (lambda sides: hub_in.at[sides], sum_send, None),
        (lambda sides: hub_x.at[sides], hub_send, paired),
    ):
        take_both("gy", piece, semaphore, also)
    take_both("gz", lambda sides: z_in.at[sides], z_send)


def local_part(sizes, nodal_scalar_values, geometry):
    comps, _, _, total = nodal_scalar_values.shape
    count = total // CHUNK
    _, groups = plan(total)
    mid_rows = offsets(groups, comps * 6)[1]
    line_rows = total // LANES * comps
    line_groups = total // (LANES * LINES)
    matrices, scales = tables()
    f32 = jnp.float32
    dma = pltpu.SemaphoreType.DMA
    any_space = pl.BlockSpec(memory_space=pl.ANY)
    return pl.pallas_call(
        functools.partial(kernel, sizes),
        out_shape=pltpu.VMEM(nodal_scalar_values.shape, f32),
        in_specs=[any_space] * 4,
        out_specs=pl.BlockSpec(memory_space=pltpu.VMEM),
        scratch_shapes=[
            pltpu.VMEM(nodal_scalar_values.shape, f32),
            pltpu.VMEM(geometry.shape, f32),
            pltpu.VMEM(matrices.shape, jnp.bfloat16),
            pltpu.VMEM(scales.shape, f32),
            pltpu.VMEM(nodal_scalar_values.shape, f32),
            pltpu.VMEM((2, comps, 8, total), f32),
            pltpu.VMEM((2, mid_rows, LANES), f32),
            pltpu.VMEM((2, mid_rows, LANES), f32),
            pltpu.VMEM((2, line_rows, LANES), f32),
            pltpu.VMEM((2, line_rows, LANES), f32),
            pltpu.VMEM((2, line_rows, LANES), f32),
            pltpu.VMEM((2, line_rows, LANES), f32),
            pltpu.VMEM((2, line_rows, LANES), f32),
            pltpu.VMEM((2, 2, line_rows, LANES), f32),
            pltpu.VMEM((2, 8, LANES), f32),
            pltpu.VMEM((2, 8, LANES), f32),
            dma((4,)),
            dma((3,)),
            dma,
            dma((count,)),
            dma,
            dma((len(groups),)),
            dma,
            dma((line_groups,)),
            dma,
            dma((line_groups,)),
            dma,
            dma((line_groups,)),
            dma,
            dma,
        ],
        compiler_params=pltpu.CompilerParams(collective_id=0, has_side_effects=True),
        name="poisson",
    )(nodal_scalar_values, geometry, jnp.asarray(matrices), jnp.asarray(scales))


def solution(mesh):
    return jax.shard_map(
        functools.partial(local_part, dict(mesh.shape)),
        mesh=mesh,
        in_specs=(P(None, "gx", "gy", "gz"), P(None, "gx", "gy", "gz")),
        out_specs=P(None, "gx", "gy", "gz"),
        check_vma=False,
    )
```

```python
import functools

import jax
import jax.numpy as jnp
import numpy as np
from jax import lax
from jax.experimental import pallas as pl
from jax.experimental.pallas import tpu as pltpu
from jax.sharding import PartitionSpec as P

interior_points = [
    -0.8717401485096066,
    -0.5917001814331423,
    -0.2092992179024789,
    0.2092992179024789,
    0.5917001814331423,
    0.8717401485096066,
]
MESH = pl.DeviceIdType.MESH
CHUNK = 256
LANES = 128
PER = CHUNK // LANES
GROUP = 4
LINES = 8


def plan(total):
    count, tiles = total // CHUNK, total // LANES
    order = [1, 2, 0, count - 1] + list(range(3, count - 1))
    late = list(range(1, count - 1)) + [0, count - 1]
    rest = [c * PER + k for c in late for k in range(PER)]
    return order, [rest[at : at + GROUP] for at in range(0, tiles, GROUP)]


def offsets(groups, rows):
    places, at = [], 0
    for group in groups:
        size = -(-len(group) * rows // 8) * 8
        places.append((at, size))
        at += size
    return places, at


def legendre_seven(point):
    previous = 1.0
    current = point
    for order in range(1, 7):
        following = ((2 * order + 1) * point * current - order * previous) / (order + 1)
        previous = current
        current = following
    return current


def gll_tables():
    degree = 7
    points = [-1.0] + interior_points + [1.0]
    values = [legendre_seven(point) for point in points]
    node_count = degree + 1
    weights = np.array([2.0 / (degree * (degree + 1) * value * value) for value in values])
    derivative = np.zeros((node_count, node_count))
    for row_index in range(node_count):
        for col_index in range(node_count):
            if row_index != col_index:
                derivative[row_index, col_index] = values[row_index] / (
                    values[col_index] * (points[row_index] - points[col_index])
                )
    derivative[0, 0] = -degree * (degree + 1) / 4.0
    derivative[node_count - 1, node_count - 1] = degree * (degree + 1) / 4.0
    return (derivative, weights)


def halves(table):
    table = np.asarray(table, np.float32)
    high = table.astype(jnp.bfloat16)
    low = (table - high.astype(np.float32)).astype(jnp.bfloat16)
    return high, low


def tables():
    derivative, weights = gll_tables()
    eye = np.eye(8)
    plane_weight = np.kron(weights, weights)
    forward_xy = np.concatenate([np.kron(derivative, eye), np.kron(eye, derivative)], axis=0)
    back_xy = np.concatenate([np.kron(derivative.T, eye), np.kron(eye, derivative.T)], axis=1)
    back_xy = back_xy * np.tile(plane_weight, 2)[None, :]
    forward_z = np.kron(np.eye(16), derivative.T)
    back_z = np.kron(np.eye(16), derivative)
    high, low = halves(forward_xy)
    forward_xy = np.concatenate([high, high, low, low], axis=1)
    high, low = halves(back_xy)
    back_xy = np.concatenate(
        [np.concatenate([high, high], axis=1), np.concatenate([low, low], axis=1)], axis=0
    )
    high, low = halves(forward_z)
    forward_z = np.concatenate([high, low], axis=1)
    high, low = halves(back_z)
    back_z = np.concatenate([high, low], axis=1)
    matrices = np.concatenate([forward_xy, back_xy, forward_z, back_z], axis=0)
    plane = np.repeat(plane_weight[:, None], LANES, axis=1)
    along = np.repeat(np.tile(weights, LANES // 8)[None, :], 8, axis=0)
    scales = np.concatenate([plane, along], axis=0).astype(np.float32)
    return matrices, scales


def split(value):
    high = value.astype(jnp.bfloat16)
    low = (value - high.astype(jnp.float32)).astype(jnp.bfloat16)
    return high, low


def product(left, right):
    return jnp.dot(left, right, preferred_element_type=jnp.float32)


def along_lanes(high, low, table):
    pieces = []
    for start in range(0, high.shape[1], LANES):
        both = jnp.concatenate(
            [high[:, start : start + LANES], low[:, start : start + LANES]], axis=1
        )
        twice = product(both, table)
        pieces.append(twice[:, :LANES] + twice[:, LANES:])
    return jnp.concatenate(pieces, axis=1)


def kernel(
    sizes,
    u_hbm,
    geo_hbm,
    mat_hbm,
    scale_hbm,
    out,
    u,
    geo,
    mat,
    scale,
    local,
    x_in,
    mid_out,
    mid_in,
    leaf_out,
    hub_own,
    hub_in,
    hub_out,
    hub_x,
    line_sum,
    z_out,
    z_in,
    in_sem,
    const_sem,
    x_send,
    x_recv,
    mid_send,
    mid_recv,
    leaf_send,
    leaf_recv,
    hub_send,
    hub_recv,
    sum_send,
    sum_recv,
    z_send,
    z_recv,
):
    comps, _, _, total = u.shape
    tiles = total // LANES
    order, groups = plan(total)
    mid_place, _ = offsets(groups, comps * 6)
    line_tiles = [tile for group in groups for tile in group]
    line_at = {tile: k for k, tile in enumerate(line_tiles)}
    line_rows = LINES * comps
    group_of = {tile: (g, k) for g, group in enumerate(groups) for k, tile in enumerate(group)}
    names = ("gx", "gy", "gz")
    place = {name: lax.axis_index(name) for name in names}
    below = {name: place[name] > 0 for name in names}
    above = {name: place[name] < sizes[name] - 1 for name in names}

    def target(name, side):
        return above[name] if side == 0 else below[name]

    def source(name, side):
        return below[name] if side == 0 else above[name]

    def when_do(condition, act):
        @pl.when(condition)
        def _():
            act()

    upper = lax.rem(place["gy"], 2)
    lower = 1 - upper
    inside = jnp.logical_and(below["gy"], above["gy"])
    facing = place["gx"] + upper - lower
    paired = jnp.logical_and(facing >= 0, facing < sizes["gx"])

    def across(side):
        return {"gx": facing, "gy": place["gy"] + (1 if side else -1)}

    barrier = pltpu.get_barrier_semaphore()
    for name in names:
        for there, by in ((below[name], -1), (above[name], 1)):

            @pl.when(there)
            def _(name=name, by=by):
                pl.semaphore_signal(
                    barrier, inc=1, device_id={name: place[name] + by}, device_id_type=MESH
                )

    greeted = sum(side[name].astype(jnp.int32) for name in names for side in (below, above))
    def in_copy(at, first, last):
        span = pl.ds(first * CHUNK, (last - first) * CHUNK)
        return pltpu.make_async_copy(
            u_hbm.at[:, :, :, span], u.at[:, :, :, span], in_sem.at[at]
        )

    count = total // CHUNK
    in_copies = [
        in_copy(0, 1, 2),
        in_copy(1, 2, count - 1),
        in_copy(2, 0, 1),
        in_copy(3, count - 1, count),
    ]
    const_copies = [
        pltpu.make_async_copy(geo_hbm, geo, const_sem.at[0]),
        pltpu.make_async_copy(scale_hbm, scale, const_sem.at[1]),
        pltpu.make_async_copy(mat_hbm, mat, const_sem.at[2]),
    ]
    in_copies[0].start()
    for copy in const_copies:
        copy.start()

    for side in range(2):

        @pl.when(jnp.logical_not(source("gx", side)))
        def _(side=side):
            x_in[side] = jnp.zeros(x_in.shape[1:], jnp.float32)

        @pl.when(jnp.logical_not(source("gy", side)))
        def _(side=side):
            mid_in[side] = jnp.zeros(mid_in.shape[1:], jnp.float32)

        @pl.when(jnp.logical_not(source("gz", side)))
        def _(side=side):
            z_in[side] = jnp.zeros(z_in.shape[1:], jnp.float32)

    @pl.when(jnp.logical_not(paired))
    def _():
        hub_x[...] = jnp.zeros(hub_x.shape, jnp.float32)

    def neighbour(name, side):
        return {name: place[name] + (1 if side == 0 else -1)}

    def x_copy(side, c, rows):
        span = pl.ds(c * CHUNK, CHUNK)
        return pltpu.make_async_remote_copy(
            local.at[:, 7 if side == 0 else 0, rows, span],
            x_in.at[side, :, rows, span],
            x_send,
            x_recv.at[line_at[c * PER] // LINES],
            device_id=neighbour("gx", side),
            device_id_type=MESH,
        )

    def mid_copy(side, g):
        span = pl.ds(*mid_place[g])
        return pltpu.make_async_remote_copy(
            mid_out.at[side, span],
            mid_in.at[side, span],
            mid_send,
            mid_recv.at[g],
            device_id=neighbour("gy", side),
            device_id_type=MESH,
        )

    def line_span(h):
        return pl.ds(h * line_rows, line_rows)

    def leaf_copy(side, h):
        return pltpu.make_async_remote_copy(
            leaf_out.at[side, line_span(h)],
            hub_in.at[side, line_span(h)],
            leaf_send,
            leaf_recv.at[h],
            device_id=neighbour("gy", side),
            device_id_type=MESH,
        )

    def hub_copy(side, h):
        return pltpu.make_async_remote_copy(
            hub_out.at[side, line_span(h)],
            hub_x.at[1 - side, line_span(h)],
            hub_send,
            hub_recv.at[h],
            device_id=across(side),
            device_id_type=MESH,
        )

    def sum_copy(side, h):
        return pltpu.make_async_remote_copy(
            line_sum.at[upper, side, line_span(h)],
            line_sum.at[upper, 1 - side, line_span(h)],
            sum_send,
            sum_recv.at[h],
            device_id={"gy": place["gy"] + (1 if side else -1)},
            device_id_type=MESH,
        )

    def z_copy(side):
        return pltpu.make_async_remote_copy(
            z_out.at[side],
            z_in.at[side],
            z_send,
            z_recv,
            device_id=neighbour("gz", side),
            device_id_type=MESH,
        )

    every = slice(None)
    within = pl.ds(1, 6)

    def take_both(name, piece, semaphore, also=None):
        both = jnp.logical_and(below[name], above[name])
        one = jnp.logical_xor(below[name], above[name])
        for condition, sides in ((both, 2), (one, 1)):
            ref = piece(pl.ds(0, sides))
            if also is not None:
                condition = jnp.logical_and(condition, also)
            when_do(condition, lambda: pltpu.make_async_copy(ref, ref, semaphore).wait())

    def take_x(span, semaphore):
        for rows, also in ((within, inside), (every, jnp.logical_not(inside))):
            take_both("gx", lambda sides: x_in.at[sides, :, rows, span], semaphore, also)

    def way(side, near):
        near_side = (upper if side else lower) > 0
        return near_side if near else jnp.logical_not(near_side)

    def send_x(c, near=None):
        for side in range(2):
            there = target("gx", side)
            if near is not None:
                there = jnp.logical_and(there, way(side, near))
            for rows, also in ((within, inside), (every, jnp.logical_not(inside))):
                when_do(jnp.logical_and(there, also), lambda: x_copy(side, c, rows).start())

    def mid_row(comp, n, tile):
        g, k = group_of[tile]
        return mid_place[g][0] + k * comps * 6 + comp * 6 + n - 1

    def line_row(comp, tile):
        return line_at[tile] * comps + comp

    for copy in const_copies[:2]:
        copy.wait()
    for copy in in_copies[1:]:
        copy.start()
    rows = jnp.concatenate(
        [geo[k, 0] for k in range(6)] + [jnp.zeros((2, geo.shape[-1]), jnp.float32)], axis=0
    )
    lane = lax.broadcasted_iota(jnp.int32, (8, LANES), 1)

    def metric_of(tile):
        first = tile * (LANES // 8)
        block = rows[:, first // LANES * LANES : first // LANES * LANES + LANES]
        spread = jnp.take_along_axis(block, lane // 8 + first % LANES, axis=1)
        return spread * scale[64:72, :]

    def compute(start, size):
        lanes = slice(start, start + size)
        metric = jnp.concatenate(
            [metric_of(start // LANES + k) for k in range(size // LANES)], axis=1
        )
        g00, g11, g22, g01, g02, g12 = [metric[k : k + 1] for k in range(6)]
        forward_xy, back_xy = mat[0:128, :], mat[128:256, :]
        forward_z = jnp.concatenate([mat[256:384, :]] * 2, axis=0)
        back_z = jnp.concatenate([mat[384:512, :]] * 2, axis=0)
        pieces = range(0, size, LANES)

        def along_all(pairs, table):
            blocks = [
                jnp.concatenate([part[:, at : at + LANES] for part in pair], axis=1)
                for pair in pairs
                for at in pieces
            ]
            twice = product(jnp.concatenate(blocks, axis=0), table)
            sums = twice[:, :LANES] + twice[:, LANES:]
            sums = [sums[64 * k : 64 * (k + 1)] for k in range(len(blocks))]
            count = len(pieces)
            return [
                jnp.concatenate(sums[k * count : (k + 1) * count], axis=1)
                for k in range(len(pairs))
            ]

        fields = [split(u[comp, :, :, lanes].reshape(64, size)) for comp in range(comps)]
        grads_z = along_all(fields, forward_z)
        partial, fluxes_z = [], []
        for comp in range(comps):
            high, low = fields[comp]
            both = product(forward_xy, jnp.concatenate([high, low, high, low], axis=0))
            grad_x, grad_y, grad_z = both[:64], both[64:], grads_z[comp]
            flux_x = g00 * grad_x + g01 * grad_y + g02 * grad_z
            flux_y = g01 * grad_x + g11 * grad_y + g12 * grad_z
            flux_z = g02 * grad_x + g12 * grad_y + g22 * grad_z
            x_high, x_low = split(flux_x)
            y_high, y_low = split(flux_y)
            fluxes_z.append(split(flux_z))
            twice = product(back_xy, jnp.concatenate([x_high, y_high, x_low, y_low], axis=0))
            partial.append(twice[:64] + twice[64:])
        weight = jnp.concatenate([scale[0:64, :]] * (size // LANES), axis=1)
        terms_z = along_all(fluxes_z, back_z)
        for comp in range(comps):
            terms = partial[comp] + weight * terms_z[comp]
            terms = terms.reshape(8, 8, size)
            local[comp, :, :, lanes] = terms
            for k in range(size // LANES):
                tile = start // LANES + k
                if tile in (0, tiles - 1):
                    continue
                part = slice(k * LANES, (k + 1) * LANES)
                for n in range(1, 7):
                    put_mid(comp, n, tile, terms[n, :, part])

    def put_mid(comp, n, tile, value):
        row = mid_row(comp, n, tile)
        mid_out[0, row : row + 1, :] = value[7:8]
        mid_out[1, row : row + 1, :] = value[0:1]

    def wait_x(h):
        take_x(pl.ds(0, LINES * LANES), x_recv.at[h])

    def send_leaf(h):
        for tile in line_tiles[h * LINES : (h + 1) * LINES]:
            lanes = slice(tile * LANES, (tile + 1) * LANES)
            for comp in range(comps):
                row = line_row(comp, tile)
                leaf = local[comp, 7 * lower, :, lanes]
                leaf_out[0, row : row + 1, :] = leaf[7:8]
                leaf_out[1, row : row + 1, :] = leaf[0:1]
                own = local[comp, 7 * upper, :, lanes]
                hub_own[0, row : row + 1, :] = own[0:1]
                hub_own[1, row : row + 1, :] = own[7:8]
        for side in range(2):
            when_do(target("gy", side), lambda: leaf_copy(side, h).start())

    def send_hub(h):
        span = line_span(h)
        take_both("gy", lambda sides: hub_in.at[sides, span], leaf_recv.at[h])
        for side in range(2):
            hub_out[side, span] = hub_own[side, span] + hub_in[side, span]
            there = jnp.logical_and(paired, source("gy", side))
            when_do(there, lambda: hub_copy(side, h).start())

    def send_sum(h):
        span = line_span(h)
        take_both("gy", lambda sides: hub_x.at[sides, span], hub_recv.at[h], paired)
        for side in range(2):
            line_sum[upper, side, span] = hub_out[side, span] + hub_x[side, span]
            when_do(source("gy", side), lambda: sum_copy(side, h).start())

    def wait_sum(h):
        take_both("gy", lambda sides: line_sum.at[lower, sides, line_span(h)], sum_recv.at[h])

    def send_mid(g, near):
        for side in range(2):
            there = jnp.logical_and(target("gy", side), way(side, near))
            when_do(there, lambda: mid_copy(side, g).start())

    def wait_mid(g):
        take_both("gy", lambda sides: mid_in.at[sides, pl.ds(*mid_place[g])], mid_recv.at[g])

    def xy_sum(comp, n, tile):
        lanes = slice(tile * LANES, (tile + 1) * LANES)
        where = lax.broadcasted_iota(jnp.int32, (8, LANES), 0)
        if n in (0, 7):
            value = local[comp, n, :, lanes] + x_in[n // 7, comp, :, lanes]
            row = line_row(comp, tile)
            first, last = [line_sum[n // 7, side, row : row + 1, :] for side in range(2)]
            value = jnp.where(where == first_line, first, value)
            return jnp.where(where == last_line, last, value)
        value = local[comp, n, :, lanes]
        row = mid_row(comp, n, tile)
        sides = [mid_in[side, row : row + 1, :] for side in range(2)]
        value = value + jnp.where(where == 0, sides[0], 0.0)
        return value + jnp.where(where == 7, sides[1], 0.0)

    first_line = jnp.where(below["gy"], 0, 8)
    last_line = jnp.where(above["gy"], 7, 8)

    def outer(side):
        return (0, 0) if side else (tiles - 1, LANES - 1)

    def send_z():
        for side in range(2):
            tile, column = outer(side)
            lanes = slice(tile * LANES, (tile + 1) * LANES)
            packed = jnp.zeros((8, LANES), jnp.float32)
            for comp in range(comps):
                for n in range(8):
                    value = local[comp, n, :, lanes][:, column : column + 1]
                    packed = jnp.where(lane == comp * 8 + n, value, packed)
            z_out[side] = packed
            when_do(target("gz", side), lambda: z_copy(side).start())

    def add_z():
        take_both("gz", lambda sides: z_in.at[sides], z_recv)
        for side in range(2):
            tile, column = outer(1 - side)
            lanes = slice(tile * LANES, (tile + 1) * LANES)
            arrived_z = z_in[side]
            for comp in range(comps):
                for n in range(8):
                    at = comp * 8 + n
                    extra = jnp.where(lane == column, arrived_z[:, at : at + 1], 0.0)
                    value = local[comp, n, :, lanes] + extra
                    local[comp, n, :, lanes] = value
                    if 0 < n < 7:
                        put_mid(comp, n, tile, value)

    def finish(which, first, last):
        for comp in range(comps):
            for n in which:
                parts = []
                for tile in range(first - 1, last + 1):
                    if 0 <= tile < tiles:
                        parts.append(xy_sum(comp, n, tile))
                    else:
                        parts.append(jnp.zeros((8, LANES), jnp.float32))
                value = jnp.concatenate(parts, axis=1)
                width = value.shape[1]
                before = pltpu.roll(value, 1, 1)[:, LANES:-LANES]
                after = pltpu.roll(value, width - 1, 1)[:, LANES:-LANES]
                position = lax.broadcasted_iota(jnp.int32, before.shape, 1) % 8
                extra = jnp.where(position == 7, after, jnp.where(position == 0, before, 0.0))
                out[comp, n, :, first * LANES : last * LANES] = value[:, LANES:-LANES] + extra

    middle, ends = range(1, 7), (0, 7)
    finished = {middle: set(), ends: set()}
    arrived = {middle: set(), ends: set()}

    def finish_ready(which):
        have = arrived[which]

        def near(tile):
            return tile in have or not 0 <= tile < tiles

        ready = [
            tile
            for tile in range(tiles)
            if tile not in finished[which] and all(near(tile + k) for k in (-1, 0, 1))
        ]
        while ready:
            first = last = ready.pop(0)
            while ready and ready[0] == last + 1 and last - first < GROUP - 1:
                last = ready.pop(0)
            finished[which].update(range(first, last + 1))
            finish(which, first, last + 1)

    const_copies[2].wait()
    for at, c in enumerate(order):
        if at < 4:
            in_copies[at].wait()
        compute(c * CHUNK, CHUNK)
        if at == 1:
            pl.semaphore_wait(barrier, greeted)
            send_x(order[0])
        if at == 3:
            send_z()
        if at == 5:
            send_leaf(0)
        if at and 0 < c < count - 2:
            send_x(c)
        if at == 1:
            send_mid(0, True)
    add_z()
    send_leaf(1)
    last = (count - 2, 0, count - 1)
    for c in last:
        send_x(c, True)

    def take_mid(g):
        wait_mid(g)
        arrived[middle].update(groups[g])
        finish_ready(middle)

    def take_ends(h):
        wait_sum(h)
        now = line_tiles[h * LINES : (h + 1) * LINES]
        wait_x(h)
        arrived[ends].update(now)
        finish_ready(ends)

    for g in (1, 2, 3):
        send_mid(g, True)
    send_hub(0)
    send_hub(1)
    for c in last:
        send_x(c, False)
    send_mid(0, False)
    send_mid(1, False)
    send_sum(0)
    send_mid(2, False)
    send_sum(1)
    send_mid(3, False)
    take_mid(0)
    take_ends(0)
    take_mid(1)
    take_mid(2)
    take_ends(1)
    take_mid(3)

    take_x(every, x_send)
    for piece, semaphore, also in (
        (lambda sides: mid_in.at[sides], mid_send, None),
        (lambda sides: hub_in.at[sides], leaf_send, None),
        (lambda sides: hub_in.at[sides], sum_send, None),
        (lambda sides: hub_x.at[sides], hub_send, paired),
    ):
        take_both("gy", piece, semaphore, also)
    take_both("gz", lambda sides: z_in.at[sides], z_send)


def local_part(sizes, nodal_scalar_values, geometry):
    comps, _, _, total = nodal_scalar_values.shape
    count = total // CHUNK
    _, groups = plan(total)
    mid_rows = offsets(groups, comps * 6)[1]
    line_rows = total // LANES * comps
    line_groups = total // (LANES * LINES)
    matrices, scales = tables()
    f32 = jnp.float32
    dma = pltpu.SemaphoreType.DMA
    any_space = pl.BlockSpec(memory_space=pl.ANY)
    return pl.pallas_call(
        functools.partial(kernel, sizes),
        out_shape=pltpu.VMEM(nodal_scalar_values.shape, f32),
        in_specs=[any_space] * 4,
        out_specs=pl.BlockSpec(memory_space=pltpu.VMEM),
        scratch_shapes=[
            pltpu.VMEM(nodal_scalar_values.shape, f32),
            pltpu.VMEM(geometry.shape, f32),
            pltpu.VMEM(matrices.shape, jnp.bfloat16),
            pltpu.VMEM(scales.shape, f32),
            pltpu.VMEM(nodal_scalar_values.shape, f32),
            pltpu.VMEM((2, comps, 8, total), f32),
            pltpu.VMEM((2, mid_rows, LANES), f32),
            pltpu.VMEM((2, mid_rows, LANES), f32),
            pltpu.VMEM((2, line_rows, LANES), f32),
            pltpu.VMEM((2, line_rows, LANES), f32),
            pltpu.VMEM((2, line_rows, LANES), f32),
            pltpu.VMEM((2, line_rows, LANES), f32),
            pltpu.VMEM((2, line_rows, LANES), f32),
            pltpu.VMEM((2, 2, line_rows, LANES), f32),
            pltpu.VMEM((2, 8, LANES), f32),
            pltpu.VMEM((2, 8, LANES), f32),
            dma((4,)),
            dma((3,)),
            dma,
            dma((line_groups,)),
            dma,
            dma((len(groups),)),
            dma,
            dma((line_groups,)),
            dma,
            dma((line_groups,)),
            dma,
            dma((line_groups,)),
            dma,
            dma,
        ],
        compiler_params=pltpu.CompilerParams(collective_id=0, has_side_effects=True),
        name="poisson",
    )(nodal_scalar_values, geometry, jnp.asarray(matrices), jnp.asarray(scales))


def solution(mesh):
    return jax.shard_map(
        functools.partial(local_part, dict(mesh.shape)),
        mesh=mesh,
        in_specs=(P(None, "gx", "gy", "gz"), P(None, "gx", "gy", "gz")),
        out_specs=P(None, "gx", "gy", "gz"),
        check_vma=False,
    )
```

```python
import functools

import jax
import jax.numpy as jnp
import numpy as np
from jax import lax
from jax.experimental import pallas as pl
from jax.experimental.pallas import tpu as pltpu
from jax.sharding import PartitionSpec as P

interior_points = [
    -0.8717401485096066,
    -0.5917001814331423,
    -0.2092992179024789,
    0.2092992179024789,
    0.5917001814331423,
    0.8717401485096066,
]
MESH = pl.DeviceIdType.MESH
CHUNK = 256
LANES = 128
PER = CHUNK // LANES
GROUP = 4
LINES = 8


def plan(total):
    count, tiles = total // CHUNK, total // LANES
    order = [1, 2, 0, count - 1] + list(range(3, count - 1))
    late = list(range(1, count - 1)) + [0, count - 1]
    rest = [c * PER + k for c in late for k in range(PER)]
    return order, [rest[at : at + GROUP] for at in range(0, tiles, GROUP)]


def offsets(groups, rows):
    places, at = [], 0
    for group in groups:
        size = -(-len(group) * rows // 8) * 8
        places.append((at, size))
        at += size
    return places, at


def legendre_seven(point):
    previous = 1.0
    current = point
    for order in range(1, 7):
        following = ((2 * order + 1) * point * current - order * previous) / (order + 1)
        previous = current
        current = following
    return current


def gll_tables():
    degree = 7
    points = [-1.0] + interior_points + [1.0]
    values = [legendre_seven(point) for point in points]
    node_count = degree + 1
    weights = np.array([2.0 / (degree * (degree + 1) * value * value) for value in values])
    derivative = np.zeros((node_count, node_count))
    for row_index in range(node_count):
        for col_index in range(node_count):
            if row_index != col_index:
                derivative[row_index, col_index] = values[row_index] / (
                    values[col_index] * (points[row_index] - points[col_index])
                )
    derivative[0, 0] = -degree * (degree + 1) / 4.0
    derivative[node_count - 1, node_count - 1] = degree * (degree + 1) / 4.0
    return (derivative, weights)


def halves(table):
    table = np.asarray(table, np.float32)
    high = table.astype(jnp.bfloat16)
    low = (table - high.astype(np.float32)).astype(jnp.bfloat16)
    return high, low


def tables():
    derivative, weights = gll_tables()
    eye = np.eye(8)
    plane_weight = np.kron(weights, weights)
    forward_xy = np.concatenate([np.kron(derivative, eye), np.kron(eye, derivative)], axis=0)
    back_xy = np.concatenate([np.kron(derivative.T, eye), np.kron(eye, derivative.T)], axis=1)
    back_xy = back_xy * np.tile(plane_weight, 2)[None, :]
    forward_z = np.kron(np.eye(16), derivative.T)
    back_z = np.kron(np.eye(16), derivative)
    high, low = halves(forward_xy)
    forward_xy = np.concatenate([high, high, low, low], axis=1)
    high, low = halves(back_xy)
    back_xy = np.concatenate(
        [np.concatenate([high, high], axis=1), np.concatenate([low, low], axis=1)], axis=0
    )
    high, low = halves(forward_z)
    forward_z = np.concatenate([high, low], axis=1)
    high, low = halves(back_z)
    back_z = np.concatenate([high, low], axis=1)
    matrices = np.concatenate([forward_xy, back_xy, forward_z, back_z], axis=0)
    plane = np.repeat(plane_weight[:, None], LANES, axis=1)
    along = np.repeat(np.tile(weights, LANES // 8)[None, :], 8, axis=0)
    scales = np.concatenate([plane, along], axis=0).astype(np.float32)
    return matrices, scales


def split(value):
    high = value.astype(jnp.bfloat16)
    low = (value - high.astype(jnp.float32)).astype(jnp.bfloat16)
    return high, low


def product(left, right):
    return jnp.dot(left, right, preferred_element_type=jnp.float32)


def along_lanes(high, low, table):
    pieces = []
    for start in range(0, high.shape[1], LANES):
        both = jnp.concatenate(
            [high[:, start : start + LANES], low[:, start : start + LANES]], axis=1
        )
        twice = product(both, table)
        pieces.append(twice[:, :LANES] + twice[:, LANES:])
    return jnp.concatenate(pieces, axis=1)


def kernel(
    sizes,
    u_hbm,
    geo_hbm,
    mat_hbm,
    scale_hbm,
    out,
    u,
    geo,
    mat,
    scale,
    local,
    x_in,
    mid_out,
    mid_in,
    leaf_out,
    hub_own,
    hub_in,
    hub_out,
    hub_x,
    line_sum,
    z_out,
    z_in,
    in_sem,
    const_sem,
    x_send,
    x_recv,
    mid_send,
    mid_recv,
    leaf_send,
    leaf_recv,
    hub_send,
    hub_recv,
    sum_send,
    sum_recv,
    z_send,
    z_recv,
):
    comps, _, _, total = u.shape
    tiles = total // LANES
    order, groups = plan(total)
    mid_place, _ = offsets(groups, comps * 6)
    line_tiles = [tile for group in groups for tile in group]
    line_at = {tile: k for k, tile in enumerate(line_tiles)}
    line_rows = LINES * comps
    group_of = {tile: (g, k) for g, group in enumerate(groups) for k, tile in enumerate(group)}
    names = ("gx", "gy", "gz")
    place = {name: lax.axis_index(name) for name in names}
    below = {name: place[name] > 0 for name in names}
    above = {name: place[name] < sizes[name] - 1 for name in names}

    def target(name, side):
        return above[name] if side == 0 else below[name]

    def source(name, side):
        return below[name] if side == 0 else above[name]

    def when_do(condition, act):
        @pl.when(condition)
        def _():
            act()

    upper = lax.rem(place["gy"], 2)
    lower = 1 - upper
    inside = jnp.logical_and(below["gy"], above["gy"])
    facing = place["gx"] + upper - lower
    paired = jnp.logical_and(facing >= 0, facing < sizes["gx"])

    def across(side):
        return {"gx": facing, "gy": place["gy"] + (1 if side else -1)}

    barrier = pltpu.get_barrier_semaphore()
    for name in names:
        for there, by in ((below[name], -1), (above[name], 1)):

            @pl.when(there)
            def _(name=name, by=by):
                pl.semaphore_signal(
                    barrier, inc=1, device_id={name: place[name] + by}, device_id_type=MESH
                )

    greeted = sum(side[name].astype(jnp.int32) for name in names for side in (below, above))
    def in_copy(at, first, last):
        span = pl.ds(first * CHUNK, (last - first) * CHUNK)
        return pltpu.make_async_copy(
            u_hbm.at[:, :, :, span], u.at[:, :, :, span], in_sem.at[at]
        )

    count = total // CHUNK
    in_copies = [
        in_copy(0, 1, 2),
        in_copy(1, 2, count - 1),
        in_copy(2, 0, 1),
        in_copy(3, count - 1, count),
    ]
    const_copies = [
        pltpu.make_async_copy(geo_hbm, geo, const_sem.at[0]),
        pltpu.make_async_copy(scale_hbm, scale, const_sem.at[1]),
        pltpu.make_async_copy(mat_hbm, mat, const_sem.at[2]),
    ]
    in_copies[0].start()
    for copy in const_copies:
        copy.start()

    for side in range(2):

        @pl.when(jnp.logical_not(source("gx", side)))
        def _(side=side):
            x_in[side] = jnp.zeros(x_in.shape[1:], jnp.float32)

        @pl.when(jnp.logical_not(source("gy", side)))
        def _(side=side):
            mid_in[side] = jnp.zeros(mid_in.shape[1:], jnp.float32)

        @pl.when(jnp.logical_not(source("gz", side)))
        def _(side=side):
            z_in[side] = jnp.zeros(z_in.shape[1:], jnp.float32)

    @pl.when(jnp.logical_not(paired))
    def _():
        hub_x[...] = jnp.zeros(hub_x.shape, jnp.float32)

    def neighbour(name, side):
        return {name: place[name] + (1 if side == 0 else -1)}

    def x_copy(side, c, rows):
        span = pl.ds(c * CHUNK, CHUNK)
        return pltpu.make_async_remote_copy(
            local.at[:, 7 if side == 0 else 0, rows, span],
            x_in.at[side, :, rows, span],
            x_send,
            x_recv.at[line_at[c * PER] // LINES],
            device_id=neighbour("gx", side),
            device_id_type=MESH,
        )

    def mid_copy(side, g):
        span = pl.ds(*mid_place[g])
        return pltpu.make_async_remote_copy(
            mid_out.at[side, span],
            mid_in.at[side, span],
            mid_send,
            mid_recv.at[g],
            device_id=neighbour("gy", side),
            device_id_type=MESH,
        )

    def line_span(h):
        return pl.ds(h * line_rows, line_rows)

    def leaf_copy(side, h):
        return pltpu.make_async_remote_copy(
            leaf_out.at[side, line_span(h)],
            hub_in.at[side, line_span(h)],
            leaf_send,
            leaf_recv.at[h],
            device_id=neighbour("gy", side),
            device_id_type=MESH,
        )

    def hub_copy(side, h):
        return pltpu.make_async_remote_copy(
            hub_out.at[side, line_span(h)],
            hub_x.at[1 - side, line_span(h)],
            hub_send,
            hub_recv.at[h],
            device_id=across(side),
            device_id_type=MESH,
        )

    def sum_copy(side, h):
        return pltpu.make_async_remote_copy(
            line_sum.at[upper, side, line_span(h)],
            line_sum.at[upper, 1 - side, line_span(h)],
            sum_send,
            sum_recv.at[h],
            device_id={"gy": place["gy"] + (1 if side else -1)},
            device_id_type=MESH,
        )

    def z_copy(side):
        return pltpu.make_async_remote_copy(
            z_out.at[side],
            z_in.at[side],
            z_send,
            z_recv,
            device_id=neighbour("gz", side),
            device_id_type=MESH,
        )

    every = slice(None)
    within = pl.ds(1, 6)

    def take_both(name, piece, semaphore, also=None):
        both = jnp.logical_and(below[name], above[name])
        one = jnp.logical_xor(below[name], above[name])
        for condition, sides in ((both, 2), (one, 1)):
            ref = piece(pl.ds(0, sides))
            if also is not None:
                condition = jnp.logical_and(condition, also)
            when_do(condition, lambda: pltpu.make_async_copy(ref, ref, semaphore).wait())

    def take_x(span, semaphore):
        for rows, also in ((within, inside), (every, jnp.logical_not(inside))):
            take_both("gx", lambda sides: x_in.at[sides, :, rows, span], semaphore, also)

    def way(side, near):
        near_side = (upper if side else lower) > 0
        return near_side if near else jnp.logical_not(near_side)

    def send_x(c, near=None):
        for side in range(2):
            there = target("gx", side)
            if near is not None:
                there = jnp.logical_and(there, way(side, near))
            for rows, also in ((within, inside), (every, jnp.logical_not(inside))):
                when_do(jnp.logical_and(there, also), lambda: x_copy(side, c, rows).start())

    def mid_row(comp, n, tile):
        g, k = group_of[tile]
        return mid_place[g][0] + k * comps * 6 + comp * 6 + n - 1

    def line_row(comp, tile):
        return line_at[tile] * comps + comp

    for copy in const_copies[:2]:
        copy.wait()
    for copy in in_copies[1:]:
        copy.start()
    rows = jnp.concatenate(
        [geo[k, 0] for k in range(6)] + [jnp.zeros((2, geo.shape[-1]), jnp.float32)], axis=0
    )
    lane = lax.broadcasted_iota(jnp.int32, (8, LANES), 1)

    def metric_of(tile):
        first = tile * (LANES // 8)
        block = rows[:, first // LANES * LANES : first // LANES * LANES + LANES]
        spread = jnp.take_along_axis(block, lane // 8 + first % LANES, axis=1)
        return spread * scale[64:72, :]

    def compute(start, size):
        lanes = slice(start, start + size)
        metric = jnp.concatenate(
            [metric_of(start // LANES + k) for k in range(size // LANES)], axis=1
        )
        g00, g11, g22, g01, g02, g12 = [metric[k : k + 1] for k in range(6)]
        forward_xy, back_xy = mat[0:128, :], mat[128:256, :]
        forward_z = jnp.concatenate([mat[256:384, :]] * 2, axis=0)
        back_z = jnp.concatenate([mat[384:512, :]] * 2, axis=0)
        pieces = range(0, size, LANES)

        def along_all(pairs, table):
            blocks = [
                jnp.concatenate([part[:, at : at + LANES] for part in pair], axis=1)
                for pair in pairs
                for at in pieces
            ]
            twice = product(jnp.concatenate(blocks, axis=0), table)
            sums = twice[:, :LANES] + twice[:, LANES:]
            sums = [sums[64 * k : 64 * (k + 1)] for k in range(len(blocks))]
            count = len(pieces)
            return [
                jnp.concatenate(sums[k * count : (k + 1) * count], axis=1)
                for k in range(len(pairs))
            ]

        fields = [split(u[comp, :, :, lanes].reshape(64, size)) for comp in range(comps)]
        grads_z = along_all(fields, forward_z)
        partial, fluxes_z = [], []
        for comp in range(comps):
            high, low = fields[comp]
            both = product(forward_xy, jnp.concatenate([high, low, high, low], axis=0))
            grad_x, grad_y, grad_z = both[:64], both[64:], grads_z[comp]
            flux_x = g00 * grad_x + g01 * grad_y + g02 * grad_z
            flux_y = g01 * grad_x + g11 * grad_y + g12 * grad_z
            flux_z = g02 * grad_x + g12 * grad_y + g22 * grad_z
            x_high, x_low = split(flux_x)
            y_high, y_low = split(flux_y)
            fluxes_z.append(split(flux_z))
            twice = product(back_xy, jnp.concatenate([x_high, y_high, x_low, y_low], axis=0))
            partial.append(twice[:64] + twice[64:])
        weight = jnp.concatenate([scale[0:64, :]] * (size // LANES), axis=1)
        terms_z = along_all(fluxes_z, back_z)
        for comp in range(comps):
            terms = partial[comp] + weight * terms_z[comp]
            terms = terms.reshape(8, 8, size)
            local[comp, :, :, lanes] = terms
            for k in range(size // LANES):
                tile = start // LANES + k
                if tile in (0, tiles - 1):
                    continue
                part = slice(k * LANES, (k + 1) * LANES)
                for n in range(1, 7):
                    put_mid(comp, n, tile, terms[n, :, part])

    def put_mid(comp, n, tile, value):
        row = mid_row(comp, n, tile)
        mid_out[0, row : row + 1, :] = value[7:8]
        mid_out[1, row : row + 1, :] = value[0:1]

    def wait_x(h):
        take_x(pl.ds(0, LINES * LANES), x_recv.at[h])

    def send_leaf(h):
        for tile in line_tiles[h * LINES : (h + 1) * LINES]:
            lanes = slice(tile * LANES, (tile + 1) * LANES)
            for comp in range(comps):
                row = line_row(comp, tile)
                leaf = local[comp, 7 * lower, :, lanes]
                leaf_out[0, row : row + 1, :] = leaf[7:8]
                leaf_out[1, row : row + 1, :] = leaf[0:1]
                own = local[comp, 7 * upper, :, lanes]
                hub_own[0, row : row + 1, :] = own[0:1]
                hub_own[1, row : row + 1, :] = own[7:8]
        for side in range(2):
            when_do(target("gy", side), lambda: leaf_copy(side, h).start())

    def send_hub(h):
        span = line_span(h)
        take_both("gy", lambda sides: hub_in.at[sides, span], leaf_recv.at[h])
        for side in range(2):
            hub_out[side, span] = hub_own[side, span] + hub_in[side, span]
            there = jnp.logical_and(paired, source("gy", side))
            when_do(there, lambda: hub_copy(side, h).start())

    def send_sum(h):
        span = line_span(h)
        take_both("gy", lambda sides: hub_x.at[sides, span], hub_recv.at[h], paired)
        for side in range(2):
            line_sum[upper, side, span] = hub_out[side, span] + hub_x[side, span]
            when_do(source("gy", side), lambda: sum_copy(side, h).start())

    def wait_sum(h):
        take_both("gy", lambda sides: line_sum.at[lower, sides, line_span(h)], sum_recv.at[h])

    def send_mid(g, near):
        for side in range(2):
            there = jnp.logical_and(target("gy", side), way(side, near))
            when_do(there, lambda: mid_copy(side, g).start())

    def wait_mid(g):
        take_both("gy", lambda sides: mid_in.at[sides, pl.ds(*mid_place[g])], mid_recv.at[g])

    def xy_sum(comp, n, tile):
        lanes = slice(tile * LANES, (tile + 1) * LANES)
        where = lax.broadcasted_iota(jnp.int32, (8, LANES), 0)
        if n in (0, 7):
            value = local[comp, n, :, lanes] + x_in[n // 7, comp, :, lanes]
            row = line_row(comp, tile)
            first, last = [line_sum[n // 7, side, row : row + 1, :] for side in range(2)]
            value = jnp.where(where == first_line, first, value)
            return jnp.where(where == last_line, last, value)
        value = local[comp, n, :, lanes]
        row = mid_row(comp, n, tile)
        sides = [mid_in[side, row : row + 1, :] for side in range(2)]
        value = value + jnp.where(where == 0, sides[0], 0.0)
        return value + jnp.where(where == 7, sides[1], 0.0)

    first_line = jnp.where(below["gy"], 0, 8)
    last_line = jnp.where(above["gy"], 7, 8)

    def outer(side):
        return (0, 0) if side else (tiles - 1, LANES - 1)

    def send_z():
        for side in range(2):
            tile, column = outer(side)
            lanes = slice(tile * LANES, (tile + 1) * LANES)
            packed = jnp.zeros((8, LANES), jnp.float32)
            for comp in range(comps):
                for n in range(8):
                    value = local[comp, n, :, lanes][:, column : column + 1]
                    packed = jnp.where(lane == comp * 8 + n, value, packed)
            z_out[side] = packed
            when_do(target("gz", side), lambda: z_copy(side).start())

    def add_z():
        take_both("gz", lambda sides: z_in.at[sides], z_recv)
        for side in range(2):
            tile, column = outer(1 - side)
            lanes = slice(tile * LANES, (tile + 1) * LANES)
            arrived_z = z_in[side]
            for comp in range(comps):
                for n in range(8):
                    at = comp * 8 + n
                    extra = jnp.where(lane == column, arrived_z[:, at : at + 1], 0.0)
                    value = local[comp, n, :, lanes] + extra
                    local[comp, n, :, lanes] = value
                    if 0 < n < 7:
                        put_mid(comp, n, tile, value)

    def finish(which, first, last):
        for comp in range(comps):
            for n in which:
                parts = []
                for tile in range(first - 1, last + 1):
                    if 0 <= tile < tiles:
                        parts.append(xy_sum(comp, n, tile))
                    else:
                        parts.append(jnp.zeros((8, LANES), jnp.float32))
                value = jnp.concatenate(parts, axis=1)
                width = value.shape[1]
                before = pltpu.roll(value, 1, 1)[:, LANES:-LANES]
                after = pltpu.roll(value, width - 1, 1)[:, LANES:-LANES]
                position = lax.broadcasted_iota(jnp.int32, before.shape, 1) % 8
                extra = jnp.where(position == 7, after, jnp.where(position == 0, before, 0.0))
                out[comp, n, :, first * LANES : last * LANES] = value[:, LANES:-LANES] + extra

    middle, ends = range(1, 7), (0, 7)
    finished = {middle: set(), ends: set()}
    arrived = {middle: set(), ends: set()}

    def finish_ready(which):
        have = arrived[which]

        def near(tile):
            return tile in have or not 0 <= tile < tiles

        ready = [
            tile
            for tile in range(tiles)
            if tile not in finished[which] and all(near(tile + k) for k in (-1, 0, 1))
        ]
        while ready:
            first = last = ready.pop(0)
            while ready and ready[0] == last + 1 and last - first < GROUP - 1:
                last = ready.pop(0)
            finished[which].update(range(first, last + 1))
            finish(which, first, last + 1)

    const_copies[2].wait()
    for at, c in enumerate(order):
        if at < 4:
            in_copies[at].wait()
        compute(c * CHUNK, CHUNK)
        if at == 0:
            pl.semaphore_wait(barrier, greeted)
        if at == 3:
            send_z()
        if at == 5:
            send_leaf(0)
        if 0 < c < count - 2:
            send_x(c)
        if at == 1:
            send_mid(0, True)
    add_z()
    send_leaf(1)
    last = (count - 2, 0, count - 1)
    for c in last:
        send_x(c, True)

    def take_mid(g):
        wait_mid(g)
        arrived[middle].update(groups[g])
        finish_ready(middle)

    def take_ends(h):
        wait_sum(h)
        now = line_tiles[h * LINES : (h + 1) * LINES]
        wait_x(h)
        arrived[ends].update(now)
        finish_ready(ends)

    for g in (1, 2, 3):
        send_mid(g, True)
    send_hub(0)
    send_hub(1)
    send_mid(0, False)
    send_mid(1, False)
    send_sum(0)
    for c in last:
        send_x(c, False)
    send_mid(2, False)
    send_sum(1)
    send_mid(3, False)
    take_mid(0)
    take_ends(0)
    take_mid(1)
    take_mid(2)
    take_ends(1)
    take_mid(3)

    take_x(every, x_send)
    for piece, semaphore, also in (
        (lambda sides: mid_in.at[sides], mid_send, None),
        (lambda sides: hub_in.at[sides], leaf_send, None),
        (lambda sides: hub_in.at[sides], sum_send, None),
        (lambda sides: hub_x.at[sides], hub_send, paired),
    ):
        take_both("gy", piece, semaphore, also)
    take_both("gz", lambda sides: z_in.at[sides], z_send)


def local_part(sizes, nodal_scalar_values, geometry):
    comps, _, _, total = nodal_scalar_values.shape
    count = total // CHUNK
    _, groups = plan(total)
    mid_rows = offsets(groups, comps * 6)[1]
    line_rows = total // LANES * comps
    line_groups = total // (LANES * LINES)
    matrices, scales = tables()
    f32 = jnp.float32
    dma = pltpu.SemaphoreType.DMA
    any_space = pl.BlockSpec(memory_space=pl.ANY)
    return pl.pallas_call(
        functools.partial(kernel, sizes),
        out_shape=pltpu.VMEM(nodal_scalar_values.shape, f32),
        in_specs=[any_space] * 4,
        out_specs=pl.BlockSpec(memory_space=pltpu.VMEM),
        scratch_shapes=[
            pltpu.VMEM(nodal_scalar_values.shape, f32),
            pltpu.VMEM(geometry.shape, f32),
            pltpu.VMEM(matrices.shape, jnp.bfloat16),
            pltpu.VMEM(scales.shape, f32),
            pltpu.VMEM(nodal_scalar_values.shape, f32),
            pltpu.VMEM((2, comps, 8, total), f32),
            pltpu.VMEM((2, mid_rows, LANES), f32),
            pltpu.VMEM((2, mid_rows, LANES), f32),
            pltpu.VMEM((2, line_rows, LANES), f32),
            pltpu.VMEM((2, line_rows, LANES), f32),
            pltpu.VMEM((2, line_rows, LANES), f32),
            pltpu.VMEM((2, line_rows, LANES), f32),
            pltpu.VMEM((2, line_rows, LANES), f32),
            pltpu.VMEM((2, 2, line_rows, LANES), f32),
            pltpu.VMEM((2, 8, LANES), f32),
            pltpu.VMEM((2, 8, LANES), f32),
            dma((4,)),
            dma((3,)),
            dma,
            dma((line_groups,)),
            dma,
            dma((len(groups),)),
            dma,
            dma((line_groups,)),
            dma,
            dma((line_groups,)),
            dma,
            dma((line_groups,)),
            dma,
            dma,
        ],
        compiler_params=pltpu.CompilerParams(collective_id=0, has_side_effects=True),
        name="poisson",
    )(nodal_scalar_values, geometry, jnp.asarray(matrices), jnp.asarray(scales))


def solution(mesh):
    return jax.shard_map(
        functools.partial(local_part, dict(mesh.shape)),
        mesh=mesh,
        in_specs=(P(None, "gx", "gy", "gz"), P(None, "gx", "gy", "gz")),
        out_specs=P(None, "gx", "gy", "gz"),
        check_vma=False,
    )
```

```python
import functools

import jax
import jax.numpy as jnp
import numpy as np
from jax import lax
from jax.experimental import pallas as pl
from jax.experimental.pallas import tpu as pltpu
from jax.sharding import PartitionSpec as P

interior_points = [
    -0.8717401485096066,
    -0.5917001814331423,
    -0.2092992179024789,
    0.2092992179024789,
    0.5917001814331423,
    0.8717401485096066,
]
MESH = pl.DeviceIdType.MESH
CHUNK = 256
LANES = 128
PER = CHUNK // LANES
GROUP = 4
LINES = 8


def plan(total):
    count, tiles = total // CHUNK, total // LANES
    order = [1, 2, 0, count - 1] + list(range(3, count - 1))
    late = list(range(1, count - 1)) + [0, count - 1]
    rest = [c * PER + k for c in late for k in range(PER)]
    return order, [rest[at : at + GROUP] for at in range(0, tiles, GROUP)]


def offsets(groups, rows):
    places, at = [], 0
    for group in groups:
        size = -(-len(group) * rows // 8) * 8
        places.append((at, size))
        at += size
    return places, at


def legendre_seven(point):
    previous = 1.0
    current = point
    for order in range(1, 7):
        following = ((2 * order + 1) * point * current - order * previous) / (order + 1)
        previous = current
        current = following
    return current


def gll_tables():
    degree = 7
    points = [-1.0] + interior_points + [1.0]
    values = [legendre_seven(point) for point in points]
    node_count = degree + 1
    weights = np.array([2.0 / (degree * (degree + 1) * value * value) for value in values])
    derivative = np.zeros((node_count, node_count))
    for row_index in range(node_count):
        for col_index in range(node_count):
            if row_index != col_index:
                derivative[row_index, col_index] = values[row_index] / (
                    values[col_index] * (points[row_index] - points[col_index])
                )
    derivative[0, 0] = -degree * (degree + 1) / 4.0
    derivative[node_count - 1, node_count - 1] = degree * (degree + 1) / 4.0
    return (derivative, weights)


def halves(table):
    table = np.asarray(table, np.float32)
    high = table.astype(jnp.bfloat16)
    low = (table - high.astype(np.float32)).astype(jnp.bfloat16)
    return high, low


def tables():
    derivative, weights = gll_tables()
    eye = np.eye(8)
    plane_weight = np.kron(weights, weights)
    forward_xy = np.concatenate([np.kron(derivative, eye), np.kron(eye, derivative)], axis=0)
    back_xy = np.concatenate([np.kron(derivative.T, eye), np.kron(eye, derivative.T)], axis=1)
    back_xy = back_xy * np.tile(plane_weight, 2)[None, :]
    forward_z = np.kron(np.eye(16), derivative.T)
    back_z = np.kron(np.eye(16), derivative)
    high, low = halves(forward_xy)
    forward_xy = np.concatenate([high, high, low, low], axis=1)
    high, low = halves(back_xy)
    back_xy = np.concatenate(
        [np.concatenate([high, high], axis=1), np.concatenate([low, low], axis=1)], axis=0
    )
    high, low = halves(forward_z)
    forward_z = np.concatenate([high, low], axis=1)
    high, low = halves(back_z)
    back_z = np.concatenate([high, low], axis=1)
    matrices = np.concatenate([forward_xy, back_xy, forward_z, back_z], axis=0)
    plane = np.repeat(plane_weight[:, None], LANES, axis=1)
    along = np.repeat(np.tile(weights, LANES // 8)[None, :], 8, axis=0)
    scales = np.concatenate([plane, along], axis=0).astype(np.float32)
    return matrices, scales


def split(value):
    high = value.astype(jnp.bfloat16)
    low = (value - high.astype(jnp.float32)).astype(jnp.bfloat16)
    return high, low


def product(left, right):
    return jnp.dot(left, right, preferred_element_type=jnp.float32)


def along_lanes(high, low, table):
    pieces = []
    for start in range(0, high.shape[1], LANES):
        both = jnp.concatenate(
            [high[:, start : start + LANES], low[:, start : start + LANES]], axis=1
        )
        twice = product(both, table)
        pieces.append(twice[:, :LANES] + twice[:, LANES:])
    return jnp.concatenate(pieces, axis=1)


def kernel(
    sizes,
    u_hbm,
    geo_hbm,
    mat_hbm,
    scale_hbm,
    out,
    u,
    geo,
    mat,
    scale,
    local,
    x_in,
    mid_out,
    mid_in,
    leaf_out,
    hub_own,
    hub_in,
    hub_out,
    hub_x,
    line_sum,
    z_out,
    z_in,
    in_sem,
    const_sem,
    x_send,
    x_recv,
    mid_send,
    mid_recv,
    leaf_recv,
    hub_send,
    hub_recv,
    sum_recv,
    z_send,
    z_recv,
):
    comps, _, _, total = u.shape
    tiles = total // LANES
    order, groups = plan(total)
    mid_place, _ = offsets(groups, comps * 6)
    line_tiles = [tile for group in groups for tile in group]
    line_at = {tile: k for k, tile in enumerate(line_tiles)}
    line_rows = LINES * comps
    group_of = {tile: (g, k) for g, group in enumerate(groups) for k, tile in enumerate(group)}
    names = ("gx", "gy", "gz")
    place = {name: lax.axis_index(name) for name in names}
    below = {name: place[name] > 0 for name in names}
    above = {name: place[name] < sizes[name] - 1 for name in names}

    def target(name, side):
        return above[name] if side == 0 else below[name]

    def source(name, side):
        return below[name] if side == 0 else above[name]

    def when_do(condition, act):
        @pl.when(condition)
        def _():
            act()

    upper = lax.rem(place["gy"], 2)
    lower = 1 - upper
    inside = jnp.logical_and(below["gy"], above["gy"])
    facing = place["gx"] + upper - lower
    paired = jnp.logical_and(facing >= 0, facing < sizes["gx"])

    def across(side):
        return {"gx": facing, "gy": place["gy"] + (1 if side else -1)}

    barrier = pltpu.get_barrier_semaphore()
    for name in names:
        for there, by in ((below[name], -1), (above[name], 1)):

            @pl.when(there)
            def _(name=name, by=by):
                pl.semaphore_signal(
                    barrier, inc=1, device_id={name: place[name] + by}, device_id_type=MESH
                )

    greeted = sum(side[name].astype(jnp.int32) for name in names for side in (below, above))
    def in_copy(at, first, last):
        span = pl.ds(first * CHUNK, (last - first) * CHUNK)
        return pltpu.make_async_copy(
            u_hbm.at[:, :, :, span], u.at[:, :, :, span], in_sem.at[at]
        )

    count = total // CHUNK
    in_copies = [
        in_copy(0, 1, 2),
        in_copy(1, 2, count - 1),
        in_copy(2, 0, 1),
        in_copy(3, count - 1, count),
    ]
    const_copies = [
        pltpu.make_async_copy(geo_hbm, geo, const_sem.at[0]),
        pltpu.make_async_copy(scale_hbm, scale, const_sem.at[1]),
        pltpu.make_async_copy(mat_hbm, mat, const_sem.at[2]),
    ]
    in_copies[0].start()
    for copy in const_copies:
        copy.start()

    for side in range(2):

        @pl.when(jnp.logical_not(source("gx", side)))
        def _(side=side):
            x_in[side] = jnp.zeros(x_in.shape[1:], jnp.float32)

        @pl.when(jnp.logical_not(source("gy", side)))
        def _(side=side):
            mid_in[side] = jnp.zeros(mid_in.shape[1:], jnp.float32)

        @pl.when(jnp.logical_not(source("gz", side)))
        def _(side=side):
            z_in[side] = jnp.zeros(z_in.shape[1:], jnp.float32)

    @pl.when(jnp.logical_not(paired))
    def _():
        hub_x[...] = jnp.zeros(hub_x.shape, jnp.float32)

    def neighbour(name, side):
        return {name: place[name] + (1 if side == 0 else -1)}

    def x_copy(side, c, rows):
        span = pl.ds(c * CHUNK, CHUNK)
        return pltpu.make_async_remote_copy(
            local.at[:, 7 if side == 0 else 0, rows, span],
            x_in.at[side, :, rows, span],
            x_send,
            x_recv.at[line_at[c * PER] // LINES],
            device_id=neighbour("gx", side),
            device_id_type=MESH,
        )

    def mid_copy(side, g):
        span = pl.ds(*mid_place[g])
        return pltpu.make_async_remote_copy(
            mid_out.at[side, span],
            mid_in.at[side, span],
            mid_send,
            mid_recv.at[g],
            device_id=neighbour("gy", side),
            device_id_type=MESH,
        )

    def line_span(h):
        return pl.ds(h * line_rows, line_rows)

    def leaf_copy(side, h):
        return pltpu.make_async_remote_copy(
            leaf_out.at[side, line_span(h)],
            hub_in.at[side, line_span(h)],
            mid_send,
            leaf_recv.at[h],
            device_id=neighbour("gy", side),
            device_id_type=MESH,
        )

    def hub_copy(side, h):
        return pltpu.make_async_remote_copy(
            hub_out.at[side, line_span(h)],
            hub_x.at[1 - side, line_span(h)],
            hub_send,
            hub_recv.at[h],
            device_id=across(side),
            device_id_type=MESH,
        )

    def sum_copy(side, h):
        return pltpu.make_async_remote_copy(
            line_sum.at[upper, side, line_span(h)],
            line_sum.at[upper, 1 - side, line_span(h)],
            mid_send,
            sum_recv.at[h],
            device_id={"gy": place["gy"] + (1 if side else -1)},
            device_id_type=MESH,
        )

    def z_copy(side):
        return pltpu.make_async_remote_copy(
            z_out.at[side],
            z_in.at[side],
            z_send,
            z_recv,
            device_id=neighbour("gz", side),
            device_id_type=MESH,
        )

    every = slice(None)
    within = pl.ds(1, 6)

    def take_both(name, piece, semaphore, also=None):
        both = jnp.logical_and(below[name], above[name])
        one = jnp.logical_xor(below[name], above[name])
        for condition, sides in ((both, 2), (one, 1)):
            ref = piece(pl.ds(0, sides))
            if also is not None:
                condition = jnp.logical_and(condition, also)
            when_do(condition, lambda: pltpu.make_async_copy(ref, ref, semaphore).wait())

    def take_x(span, semaphore):
        for rows, also in ((within, inside), (every, jnp.logical_not(inside))):
            take_both("gx", lambda sides: x_in.at[sides, :, rows, span], semaphore, also)

    def way(side, near):
        near_side = (upper if side else lower) > 0
        return near_side if near else jnp.logical_not(near_side)

    def send_x(c, near=None):
        for side in range(2):
            there = target("gx", side)
            if near is not None:
                there = jnp.logical_and(there, way(side, near))
            for rows, also in ((within, inside), (every, jnp.logical_not(inside))):
                when_do(jnp.logical_and(there, also), lambda: x_copy(side, c, rows).start())

    def mid_row(comp, n, tile):
        g, k = group_of[tile]
        return mid_place[g][0] + k * comps * 6 + comp * 6 + n - 1

    def line_row(comp, tile):
        return line_at[tile] * comps + comp

    for copy in const_copies[:2]:
        copy.wait()
    for copy in in_copies[1:]:
        copy.start()
    rows = jnp.concatenate(
        [geo[k, 0] for k in range(6)] + [jnp.zeros((2, geo.shape[-1]), jnp.float32)], axis=0
    )
    lane = lax.broadcasted_iota(jnp.int32, (8, LANES), 1)

    def metric_of(tile):
        first = tile * (LANES // 8)
        block = rows[:, first // LANES * LANES : first // LANES * LANES + LANES]
        spread = jnp.take_along_axis(block, lane // 8 + first % LANES, axis=1)
        return spread * scale[64:72, :]

    def compute(start, size):
        lanes = slice(start, start + size)
        metric = jnp.concatenate(
            [metric_of(start // LANES + k) for k in range(size // LANES)], axis=1
        )
        g00, g11, g22, g01, g02, g12 = [metric[k : k + 1] for k in range(6)]
        forward_xy, back_xy = mat[0:128, :], mat[128:256, :]
        forward_z = jnp.concatenate([mat[256:384, :]] * 2, axis=0)
        back_z = jnp.concatenate([mat[384:512, :]] * 2, axis=0)
        pieces = range(0, size, LANES)

        def along_all(pairs, table):
            blocks = [
                jnp.concatenate([part[:, at : at + LANES] for part in pair], axis=1)
                for pair in pairs
                for at in pieces
            ]
            twice = product(jnp.concatenate(blocks, axis=0), table)
            sums = twice[:, :LANES] + twice[:, LANES:]
            sums = [sums[64 * k : 64 * (k + 1)] for k in range(len(blocks))]
            count = len(pieces)
            return [
                jnp.concatenate(sums[k * count : (k + 1) * count], axis=1)
                for k in range(len(pairs))
            ]

        fields = [split(u[comp, :, :, lanes].reshape(64, size)) for comp in range(comps)]
        grads_z = along_all(fields, forward_z)
        partial, fluxes_z = [], []
        for comp in range(comps):
            high, low = fields[comp]
            both = product(forward_xy, jnp.concatenate([high, low, high, low], axis=0))
            grad_x, grad_y, grad_z = both[:64], both[64:], grads_z[comp]
            flux_x = g00 * grad_x + g01 * grad_y + g02 * grad_z
            flux_y = g01 * grad_x + g11 * grad_y + g12 * grad_z
            flux_z = g02 * grad_x + g12 * grad_y + g22 * grad_z
            x_high, x_low = split(flux_x)
            y_high, y_low = split(flux_y)
            fluxes_z.append(split(flux_z))
            twice = product(back_xy, jnp.concatenate([x_high, y_high, x_low, y_low], axis=0))
            partial.append(twice[:64] + twice[64:])
        weight = jnp.concatenate([scale[0:64, :]] * (size // LANES), axis=1)
        terms_z = along_all(fluxes_z, back_z)
        for comp in range(comps):
            terms = partial[comp] + weight * terms_z[comp]
            terms = terms.reshape(8, 8, size)
            local[comp, :, :, lanes] = terms
            for k in range(size // LANES):
                tile = start // LANES + k
                if tile in (0, tiles - 1):
                    continue
                part = slice(k * LANES, (k + 1) * LANES)
                for n in range(1, 7):
                    put_mid(comp, n, tile, terms[n, :, part])

    def put_mid(comp, n, tile, value):
        row = mid_row(comp, n, tile)
        mid_out[0, row : row + 1, :] = value[7:8]
        mid_out[1, row : row + 1, :] = value[0:1]

    def wait_x(h):
        take_x(pl.ds(0, LINES * LANES), x_recv.at[h])

    def send_leaf(h):
        for tile in line_tiles[h * LINES : (h + 1) * LINES]:
            lanes = slice(tile * LANES, (tile + 1) * LANES)
            for comp in range(comps):
                row = line_row(comp, tile)
                leaf = local[comp, 7 * lower, :, lanes]
                leaf_out[0, row : row + 1, :] = leaf[7:8]
                leaf_out[1, row : row + 1, :] = leaf[0:1]
                own = local[comp, 7 * upper, :, lanes]
                hub_own[0, row : row + 1, :] = own[0:1]
                hub_own[1, row : row + 1, :] = own[7:8]
        for side in range(2):
            when_do(target("gy", side), lambda: leaf_copy(side, h).start())

    def send_hub(h):
        span = line_span(h)
        take_both("gy", lambda sides: hub_in.at[sides, span], leaf_recv.at[h])
        for side in range(2):
            hub_out[side, span] = hub_own[side, span] + hub_in[side, span]
            there = jnp.logical_and(paired, source("gy", side))
            when_do(there, lambda: hub_copy(side, h).start())

    def send_sum(h):
        span = line_span(h)
        take_both("gy", lambda sides: hub_x.at[sides, span], hub_recv.at[h], paired)
        for side in range(2):
            line_sum[upper, side, span] = hub_out[side, span] + hub_x[side, span]
            when_do(source("gy", side), lambda: sum_copy(side, h).start())

    def wait_sum(h):
        take_both("gy", lambda sides: line_sum.at[lower, sides, line_span(h)], sum_recv.at[h])

    def send_mid(g, near):
        for side in range(2):
            there = jnp.logical_and(target("gy", side), way(side, near))
            when_do(there, lambda: mid_copy(side, g).start())

    def wait_mid(g):
        take_both("gy", lambda sides: mid_in.at[sides, pl.ds(*mid_place[g])], mid_recv.at[g])

    def xy_sum(comp, n, tile):
        lanes = slice(tile * LANES, (tile + 1) * LANES)
        where = lax.broadcasted_iota(jnp.int32, (8, LANES), 0)
        if n in (0, 7):
            value = local[comp, n, :, lanes] + x_in[n // 7, comp, :, lanes]
            row = line_row(comp, tile)
            first, last = [line_sum[n // 7, side, row : row + 1, :] for side in range(2)]
            value = jnp.where(where == first_line, first, value)
            return jnp.where(where == last_line, last, value)
        value = local[comp, n, :, lanes]
        row = mid_row(comp, n, tile)
        sides = [mid_in[side, row : row + 1, :] for side in range(2)]
        value = value + jnp.where(where == 0, sides[0], 0.0)
        return value + jnp.where(where == 7, sides[1], 0.0)

    first_line = jnp.where(below["gy"], 0, 8)
    last_line = jnp.where(above["gy"], 7, 8)

    def outer(side):
        return (0, 0) if side else (tiles - 1, LANES - 1)

    def send_z():
        for side in range(2):
            tile, column = outer(side)
            lanes = slice(tile * LANES, (tile + 1) * LANES)
            packed = jnp.zeros((8, LANES), jnp.float32)
            for comp in range(comps):
                for n in range(8):
                    value = local[comp, n, :, lanes][:, column : column + 1]
                    packed = jnp.where(lane == comp * 8 + n, value, packed)
            z_out[side] = packed
            when_do(target("gz", side), lambda: z_copy(side).start())

    def add_z():
        take_both("gz", lambda sides: z_in.at[sides], z_recv)
        for side in range(2):
            tile, column = outer(1 - side)
            lanes = slice(tile * LANES, (tile + 1) * LANES)
            arrived_z = z_in[side]
            for comp in range(comps):
                for n in range(8):
                    at = comp * 8 + n
                    extra = jnp.where(lane == column, arrived_z[:, at : at + 1], 0.0)
                    value = local[comp, n, :, lanes] + extra
                    local[comp, n, :, lanes] = value
                    if 0 < n < 7:
                        put_mid(comp, n, tile, value)

    def finish(which, first, last):
        for comp in range(comps):
            for n in which:
                parts = []
                for tile in range(first - 1, last + 1):
                    if 0 <= tile < tiles:
                        parts.append(xy_sum(comp, n, tile))
                    else:
                        parts.append(jnp.zeros((8, LANES), jnp.float32))
                value = jnp.concatenate(parts, axis=1)
                width = value.shape[1]
                before = pltpu.roll(value, 1, 1)[:, LANES:-LANES]
                after = pltpu.roll(value, width - 1, 1)[:, LANES:-LANES]
                position = lax.broadcasted_iota(jnp.int32, before.shape, 1) % 8
                extra = jnp.where(position == 7, after, jnp.where(position == 0, before, 0.0))
                out[comp, n, :, first * LANES : last * LANES] = value[:, LANES:-LANES] + extra

    middle, ends = range(1, 7), (0, 7)
    finished = {middle: set(), ends: set()}
    arrived = {middle: set(), ends: set()}

    def finish_ready(which):
        have = arrived[which]

        def near(tile):
            return tile in have or not 0 <= tile < tiles

        ready = [
            tile
            for tile in range(tiles)
            if tile not in finished[which] and all(near(tile + k) for k in (-1, 0, 1))
        ]
        while ready:
            first = last = ready.pop(0)
            while ready and ready[0] == last + 1 and last - first < GROUP - 1:
                last = ready.pop(0)
            finished[which].update(range(first, last + 1))
            finish(which, first, last + 1)

    const_copies[2].wait()
    for at, c in enumerate(order):
        if at < 4:
            in_copies[at].wait()
        compute(c * CHUNK, CHUNK)
        if at == 0:
            pl.semaphore_wait(barrier, greeted)
        if at == 3:
            send_z()
        if at == 5:
            send_leaf(0)
        if 0 < c < count - 2:
            send_x(c)
        if at == 1:
            send_mid(0, True)
    add_z()
    send_leaf(1)
    last = (count - 2, 0, count - 1)
    for c in last:
        send_x(c, True)

    def take_mid(g):
        wait_mid(g)
        arrived[middle].update(groups[g])
        finish_ready(middle)

    def take_ends(h):
        wait_sum(h)
        now = line_tiles[h * LINES : (h + 1) * LINES]
        wait_x(h)
        arrived[ends].update(now)
        finish_ready(ends)

    for g in (1, 2, 3):
        send_mid(g, True)
    send_hub(0)
    send_hub(1)
    send_mid(0, False)
    send_mid(1, False)
    send_sum(0)
    for c in last:
        send_x(c, False)
    send_mid(2, False)
    send_sum(1)
    send_mid(3, False)
    take_mid(0)
    take_mid(1)
    take_ends(0)
    take_mid(2)
    take_ends(1)
    take_mid(3)

    take_x(every, x_send)
    for piece, semaphore, also in (
        (lambda sides: x_in.at[sides], mid_send, None),
        (lambda sides: hub_x.at[sides], hub_send, paired),
    ):
        take_both("gy", piece, semaphore, also)
    take_both("gz", lambda sides: z_in.at[sides], z_send)


def local_part(sizes, nodal_scalar_values, geometry):
    comps, _, _, total = nodal_scalar_values.shape
    count = total // CHUNK
    _, groups = plan(total)
    mid_rows = offsets(groups, comps * 6)[1]
    line_rows = total // LANES * comps
    line_groups = total // (LANES * LINES)
    matrices, scales = tables()
    f32 = jnp.float32
    dma = pltpu.SemaphoreType.DMA
    any_space = pl.BlockSpec(memory_space=pl.ANY)
    return pl.pallas_call(
        functools.partial(kernel, sizes),
        out_shape=pltpu.VMEM(nodal_scalar_values.shape, f32),
        in_specs=[any_space] * 4,
        out_specs=pl.BlockSpec(memory_space=pltpu.VMEM),
        scratch_shapes=[
            pltpu.VMEM(nodal_scalar_values.shape, f32),
            pltpu.VMEM(geometry.shape, f32),
            pltpu.VMEM(matrices.shape, jnp.bfloat16),
            pltpu.VMEM(scales.shape, f32),
            pltpu.VMEM(nodal_scalar_values.shape, f32),
            pltpu.VMEM((2, comps, 8, total), f32),
            pltpu.VMEM((2, mid_rows, LANES), f32),
            pltpu.VMEM((2, mid_rows, LANES), f32),
            pltpu.VMEM((2, line_rows, LANES), f32),
            pltpu.VMEM((2, line_rows, LANES), f32),
            pltpu.VMEM((2, line_rows, LANES), f32),
            pltpu.VMEM((2, line_rows, LANES), f32),
            pltpu.VMEM((2, line_rows, LANES), f32),
            pltpu.VMEM((2, 2, line_rows, LANES), f32),
            pltpu.VMEM((2, 8, LANES), f32),
            pltpu.VMEM((2, 8, LANES), f32),
            dma((4,)),
            dma((3,)),
            dma,
            dma((line_groups,)),
            dma,
            dma((len(groups),)),
            dma((line_groups,)),
            dma,
            dma((line_groups,)),
            dma((line_groups,)),
            dma,
            dma,
        ],
        compiler_params=pltpu.CompilerParams(collective_id=0, has_side_effects=True),
        name="poisson",
    )(nodal_scalar_values, geometry, jnp.asarray(matrices), jnp.asarray(scales))


def solution(mesh):
    return jax.shard_map(
        functools.partial(local_part, dict(mesh.shape)),
        mesh=mesh,
        in_specs=(P(None, "gx", "gy", "gz"), P(None, "gx", "gy", "gz")),
        out_specs=P(None, "gx", "gy", "gz"),
        check_vma=False,
    )
```
